32 devices in a mesh: seq: 8 (over z, x), tp: 4 (over y, core).
Axes of the slice: x: 2, y: 2, z: 4, core: 2. Of those that a mesh axis runs over, the one named last changes fastest.
Arguments:
- query: bfloat16 [4096, 2048], P('seq', 'tp'), may hold values from -6 to 6
- keys: bfloat16 [4096, 2048], P('seq', 'tp'), may hold values from -6 to 6
- values: bfloat16 [4096, 2048], P('seq', 'tp'), may hold values from -7 to 7
- beta: float32 [16], P('tp'), may hold values from -2 to 2
- out_weight: bfloat16 [2048, 2048], P('tp'), may hold values from -0.125 to 0.125
- cotangent: bfloat16 [4096, 2048], P(('seq', 'tp')), may hold values from -6 to 6
Outputs:
- output: bfloat16 [4096, 2048], P(('seq', 'tp'))
- grad_query: bfloat16 [4096, 2048], P('seq', 'tp')
- grad_keys: bfloat16 [4096, 2048], P('seq', 'tp')
- grad_values: bfloat16 [4096, 2048], P('seq', 'tp')
The draws below stay inside these ranges and needn't reach their ends.
All inputs are finite; a program needn't handle non-finite values.
Results may differ from the reference program's by a relative error of at most 0.0055.
The reference program's roundings to bfloat16 on the way (of `probs_b`, `mixed`, `grad_mixed`, `grad_local` and `grad_scores`) count: a program that leaves them out, or rounds other values in their place, can miss the bound.
Values may be sent and summed in bfloat16 or wider, within the bound.
No kernel may reach another device: no remote copies, remote signals or barrier semaphores. Data moves between devices by JAX's collectives and lax.ppermute only.
A program may use at most 128 MiB of HBM per device.

```python
import jax
import jax.numpy as jnp
from jax import lax

D = 2048
HEADS = 16
HD = 128
TOK_DEV = 512
TOKENS = 4096


def query_and_keys(key):
    width = HEADS * HD
    first = jax.random.fold_in(key, 11)
    second = jax.random.fold_in(key, 12)
    query_out = jnp.clip(jax.random.normal(first, (TOKENS, width), jnp.float32), -4.0, 4.0)
    keys_out = jnp.clip(jax.random.normal(second, (TOKENS, width), jnp.float32), -4.0, 4.0)
    return (query_out, keys_out)


def draw_query(key, part):
    return query_and_keys(key)[0].astype(jnp.bfloat16)


def draw_keys(key, part):
    return query_and_keys(key)[1].astype(jnp.bfloat16)


def draw_values(key, part):
    width = HEADS * HD
    segment_count = TOKENS // TOK_DEV
    first = jax.random.fold_in(key, 21)
    second = jax.random.fold_in(key, 22)
    noise = jnp.clip(jax.random.normal(first, (segment_count, TOK_DEV, width), jnp.float32), -4.0, 4.0)
    means = jnp.clip(jax.random.normal(second, (segment_count, 1, width), jnp.float32), -3.0, 3.0)
    return (noise + means).reshape(TOKENS, width).astype(jnp.bfloat16)


def block_scale(own_key, dims, shards, least, top_value):
    gain, own = 1.0, jax.random.fold_in(own_key, 6)
    for dim, blocks in shards:
        heights = jnp.exp(jax.random.uniform(jax.random.fold_in(own, dim), (blocks,), jnp.float32, least / len(shards), top_value / len(shards)))
        gain = gain * jnp.repeat(heights, dims[dim] // blocks).reshape([-1 if axis == dim else 1 for axis in range(len(dims))])
    return gain


def bell_draw(own_key, dims, scale, most, split=(), held_as=jnp.bfloat16):
    entries = jax.random.normal(own_key, dims, jnp.float32) * scale
    if len(split) > 0:
        entries = block_scale(own_key, dims, split, -0.22, 0.18) * entries
    return jnp.clip(entries, min=-most, max=most).astype(held_as)


def setup_inputs(seed: int = 0) -> dict:
    arg_keys = jax.random.split(jax.random.key(seed), 7)
    return {
        "query": draw_query(jax.random.fold_in(arg_keys[6], 71), 0),
        "keys": draw_keys(jax.random.fold_in(arg_keys[6], 71), 0),
        "values": draw_values(jax.random.fold_in(arg_keys[6], 71), 0),
        "beta": jnp.clip(jax.random.uniform(arg_keys[3], (HEADS,), jnp.float32, -2.0, 2.0) * block_scale(arg_keys[3], (HEADS,), ((0, 4),), -0.4, 0.0), -2.0, 2.0),
        "out_weight": bell_draw(arg_keys[4], (HEADS * HD, D), (HEADS * HD) ** -0.5, 0.125, ((0, 4),)),
        "cotangent": bell_draw(arg_keys[5], (TOKENS, D), 1.0, 6.0, ((0, 32),)),
    }


highest = lax.Precision.HIGHEST

def plus_one(inputs):
    return jnp.where(inputs > 0, inputs + 1.0, jnp.exp(jnp.minimum(inputs, 0.0)))

def slope_of(inputs):
    return jnp.where(inputs > 0, jnp.ones_like(inputs), jnp.exp(jnp.minimum(inputs, 0.0)))

def batched(form, left, right):
    return jnp.einsum(form, left.astype(jnp.float32), right.astype(jnp.float32), precision=highest, preferred_element_type=jnp.float32)

def local_memory(keys_seg, values_seg):
    key_feat = plus_one(keys_seg.astype(jnp.float32))
    return (batched('lhc,lhd->hcd', key_feat, values_seg), lax.optimization_barrier(jnp.sum(key_feat, 0)))

def attention_probs(query_seg, keys_seg):
    length = query_seg.shape[0]
    scores = batched('lhc,mhc->hlm', query_seg, keys_seg) * HD ** (-0.5)
    causal = jnp.arange(length)[:, None] >= jnp.arange(length)[None, :]
    scores = jnp.where(causal[None], scores, -jnp.inf)
    top_score = lax.optimization_barrier(jnp.max(scores, -1, keepdims=True))
    expo = jnp.exp(scores - top_score)
    return expo / lax.optimization_barrier(jnp.sum(expo, -1, keepdims=True))

def memory_read(query_seg, memory, memory_sum):
    query_feat = plus_one(query_seg.astype(jnp.float32))
    numer = batched('lhc,hcd->lhd', query_feat, memory)
    denom = batched('lhc,hc->lh', query_feat, memory_sum) + 1.0
    return (query_feat, numer / denom[..., None], denom)

def segment_forward(query_seg, keys_seg, values_seg, memory, memory_sum, gate_mix):
    probs_b = attention_probs(query_seg, keys_seg).astype(jnp.bfloat16)
    local_out = batched('hlm,mhc->lhc', probs_b, values_seg)
    query_feat, mem_out, denom = memory_read(query_seg, memory, memory_sum)
    mixed = gate_mix[None, :, None] * mem_out + (1.0 - gate_mix)[None, :, None] * local_out
    return mixed.astype(jnp.bfloat16)

def memory_grads(query_seg, memory, memory_sum, grad_b, gate_mix):
    query_feat, mem_out, denom = memory_read(query_seg, memory, memory_sum)
    grad_mem = gate_mix[None, :, None] * grad_b.astype(jnp.float32)
    grad_numer = grad_mem / denom[..., None]
    grad_denom = -lax.optimization_barrier(jnp.sum(grad_mem * mem_out, -1)) / denom
    return (query_feat, grad_numer, grad_denom)

def segment_memory_grad(query_seg, memory, memory_sum, grad_b, gate_mix):
    query_feat, grad_numer, grad_denom = memory_grads(query_seg, memory, memory_sum, grad_b, gate_mix)
    return (batched('lhc,lhd->hcd', query_feat, grad_numer), batched('lh,lhc->hc', grad_denom, query_feat))

def segment_backward(query_seg, keys_seg, values_seg, memory, memory_sum, later_memory, later_sum, grad_b, gate_mix):
    probs = attention_probs(query_seg, keys_seg)
    probs_b = probs.astype(jnp.bfloat16)
    grad_local = ((1.0 - gate_mix)[None, :, None] * grad_b.astype(jnp.float32)).astype(jnp.bfloat16)
    grad_probs = batched('lhc,mhc->hlm', grad_local, values_seg)
    delta = lax.optimization_barrier(jnp.sum(probs * grad_probs, -1, keepdims=True))
    grad_scores = (probs * (grad_probs - delta) * HD ** (-0.5)).astype(jnp.bfloat16)
    query_local = batched('hlm,mhc->lhc', grad_scores, keys_seg)
    keys_local = batched('hlm,lhc->mhc', grad_scores, query_seg)
    values_local = batched('hlm,lhc->mhc', probs_b, grad_local)
    query_feat, grad_numer, grad_denom = memory_grads(query_seg, memory, memory_sum, grad_b, gate_mix)
    grad_qfeat = batched('lhd,hcd->lhc', grad_numer, memory) + grad_denom[..., None] * memory_sum[None]
    key_feat = plus_one(keys_seg.astype(jnp.float32))
    grad_kfeat = batched('lhd,hcd->lhc', values_seg, later_memory) + later_sum[None]
    values_mem = batched('lhc,hcd->lhd', key_feat, later_memory)
    grad_query = (query_local + grad_qfeat * slope_of(query_seg.astype(jnp.float32))).astype(jnp.bfloat16)
    grad_keys = (keys_local + grad_kfeat * slope_of(keys_seg.astype(jnp.float32))).astype(jnp.bfloat16)
    grad_values = (values_local + values_mem).astype(jnp.bfloat16)
    return (grad_query, grad_keys, grad_values)

def reference(query, keys, values, beta, out_weight, cotangent):
    segment_count = TOKENS // TOK_DEV

    def shaped(tensor):
        return tensor.reshape(segment_count, TOK_DEV, HEADS, HD)
    query_s, keys_s, values_s = (shaped(query), shaped(keys), shaped(values))
    gate_mix = jax.nn.sigmoid(beta.astype(jnp.float32))
    own_memory, own_sum = lax.map(lambda block: local_memory(block[0], block[1]), (keys_s, values_s))
    memory = jnp.concatenate([jnp.zeros_like(own_memory[:1]), jnp.cumsum(own_memory, 0)[:-1]], 0)
    memory_sum = jnp.concatenate([jnp.zeros_like(own_sum[:1]), jnp.cumsum(own_sum, 0)[:-1]], 0)
    mixed = lax.map(lambda block: segment_forward(block[0], block[1], block[2], block[3], block[4], gate_mix), (query_s, keys_s, values_s, memory, memory_sum))
    flat = mixed.reshape(TOKENS, HEADS * HD)
    output = jnp.dot(flat, out_weight, preferred_element_type=jnp.float32).astype(jnp.bfloat16)
    grad_mixed = lax.dot_general(cotangent, out_weight, (((1,), (1,)), ((), ())), preferred_element_type=jnp.float32).astype(jnp.bfloat16)
    grad_s = shaped(grad_mixed)
    memory_grad, sum_grad = lax.map(lambda block: segment_memory_grad(block[0], block[1], block[2], block[3], gate_mix), (query_s, memory, memory_sum, grad_s))
    later_memory = jnp.concatenate([jnp.cumsum(memory_grad[::-1], 0)[::-1][1:], jnp.zeros_like(memory_grad[:1])], 0)
    later_sum = jnp.concatenate([jnp.cumsum(sum_grad[::-1], 0)[::-1][1:], jnp.zeros_like(sum_grad[:1])], 0)
    grad_query, grad_keys, grad_values = lax.map(lambda block: segment_backward(block[0], block[1], block[2], block[3], block[4], block[5], block[6], block[7], gate_mix), (query_s, keys_s, values_s, memory, memory_sum, later_memory, later_sum, grad_s))
    width = HEADS * HD
    return (output, grad_query.reshape(TOKENS, width), grad_keys.reshape(TOKENS, width), grad_values.reshape(TOKENS, width))
```

```python
import functools

import jax
import jax.numpy as jnp
from jax import lax
from jax.experimental import pallas as pl
from jax.experimental.pallas import tpu as pltpu
from jax.sharding import PartitionSpec as P

HD = 128
PAD = 16
SCALE = HD ** (-0.5)

f32 = jnp.float32
bf16 = jnp.bfloat16

VM = pl.BlockSpec(memory_space=pltpu.VMEM)
SM = pl.BlockSpec(memory_space=pltpu.SMEM)


def dot(a, b, ca, cb):
    return lax.dot_general(a, b, (((ca,), (cb,)), ((), ())), preferred_element_type=f32)


def split(x):
    hi = x.astype(bf16)
    return hi, (x - hi.astype(f32)).astype(bf16)


def feat(x):
    return jnp.where(x > 0, x + 1.0, jnp.exp(jnp.minimum(x, 0.0)))


def slope(x):
    return jnp.where(x > 0, 1.0, jnp.exp(jnp.minimum(x, 0.0)))


def gate(beta_ref, h):
    return jax.nn.sigmoid(jnp.full((1, HD), beta_ref[h], f32))


def cols(h):
    return slice(h * HD, (h + 1) * HD)


def call(body, outs, specs, out_specs=None, scratch=(), flops=1 << 28, trans=0, name=None, vmem=40):
    if out_specs is None:
        out_specs = [VM] * len(outs)
    return pl.pallas_call(
        body,
        out_shape=[jax.ShapeDtypeStruct(s, d) for s, d in outs],
        in_specs=specs,
        out_specs=out_specs,
        scratch_shapes=list(scratch),
        compiler_params=pltpu.CompilerParams(vmem_limit_bytes=vmem << 20),
        cost_estimate=pl.CostEstimate(flops=flops, transcendentals=trans, bytes_accessed=1 << 20),
        name=name,
    )


def pad_rows(rows):
    return jnp.concatenate(rows + [jnp.zeros((PAD - len(rows), HD), f32)], 0).astype(bf16)


def own_memory_body(heads, k_ref, v_ref, o_ref):
    rows = []
    for h in range(heads):
        kf = feat(k_ref[:, cols(h)].astype(f32))
        hi, lo = split(kf)
        v = v_ref[:, cols(h)]
        o_ref[cols(h), :] = (dot(hi, v, 0, 0) + dot(lo, v, 0, 0)).astype(bf16)
        rows.append(jnp.sum(kf, 0, keepdims=True))
    o_ref[heads * HD :, :] = pad_rows(rows)


def read_memory(qf, mem_ref, heads, h):
    qh, ql = split(qf)
    mh, ml = split(mem_ref[cols(h), :])
    msum = mem_ref[heads * HD + h : heads * HD + h + 1, :]
    numer = dot(qh, mh, 1, 0) + dot(ql, mh, 1, 0) + dot(qh, ml, 1, 0)
    denom = jnp.sum(qf * msum, 1, keepdims=True) + 1.0
    r = 1.0 / denom
    return numer * r, r, mh, ml, msum


def probs_parts(q_ref, k_ref, h, j, block):
    q = q_ref[j * block : (j + 1) * block, cols(h)]
    parts = []
    for i in range(j + 1):
        k = k_ref[i * block : (i + 1) * block, cols(h)]
        s = dot(k, q, 1, 1) * SCALE
        if i == j:
            shape = (block, block)
            keep = lax.broadcasted_iota(jnp.int32, shape, 0) <= lax.broadcasted_iota(jnp.int32, shape, 1)
            s = jnp.where(keep, s, -jnp.inf)
        parts.append(s)
    top = functools.reduce(jnp.maximum, [jnp.max(s, 0, keepdims=True) for s in parts])
    parts = [jnp.exp(s - top) for s in parts]
    r = 1.0 / sum(jnp.sum(e, 0, keepdims=True) for e in parts)
    return q, [e * r for e in parts]


def local_forward_body(heads, block, q_ref, k_ref, v_ref, o_ref):
    for h in range(heads):
        vt = v_ref[:, cols(h)].T
        for j in range(q_ref.shape[0] // block):
            _, parts = probs_parts(q_ref, k_ref, h, j, block)
            acc = sum(
                dot(vt[:, i * block : (i + 1) * block], p.astype(bf16), 1, 0) for i, p in enumerate(parts)
            )
            o_ref[j * block : (j + 1) * block, cols(h)] = acc.T


def grad_mixed_body(count, place_ref, *refs):
    pieces, w_ref, o_ref, all_ref = refs[:count], refs[count], refs[count + 1], refs[count + 2]
    rows = pieces[0].shape[0]
    for i, piece in enumerate(pieces):
        spot = pl.multiple_of(place_ref[i] * rows, rows)
        all_ref[pl.ds(spot, rows), :] = piece[...]
    o_ref[...] = dot(all_ref[...], w_ref[...], 1, 1).astype(bf16)


def memory_grad_body(heads, q_ref, mem_ref, g_ref, beta_ref, o_ref):
    rows = []
    for h in range(heads):
        qf = feat(q_ref[:, cols(h)].astype(f32))
        mem_out, r, _, _, _ = read_memory(qf, mem_ref, heads, h)
        gmem = gate(beta_ref, h) * g_ref[:, cols(h)].astype(f32)
        nh, nl = split(gmem * r)
        gden = -jnp.sum(gmem * mem_out, 1, keepdims=True) * r
        qh, ql = split(qf)
        o_ref[cols(h), :] = (dot(qh, nh, 0, 0) + dot(ql, nh, 0, 0) + dot(qh, nl, 0, 0)).astype(bf16)
        rows.append(jnp.sum(gden * qf, 0, keepdims=True))
    o_ref[heads * HD :, :] = pad_rows(rows)


def output_body(heads, count, place_ref, q_ref, mem_ref, lo_ref, beta_ref, w_ref, send_ref, keep_ref, mix_ref):
    for h in range(heads):
        qf = feat(q_ref[:, cols(h)].astype(f32))
        mem_out = read_memory(qf, mem_ref, heads, h)[0]
        g = gate(beta_ref, h)
        mix_ref[:, cols(h)] = (g * mem_out + (1.0 - g) * lo_ref[:, cols(h)]).astype(bf16)
    rows = q_ref.shape[0] // count
    half = count // 2

    def gathered(first):
        out = []
        for i in range(first, first + half):
            spot = pl.multiple_of(place_ref[i] * rows, rows)
            out.append(mix_ref[pl.ds(spot, rows), :])
        return jnp.concatenate(out, 0)

    send_ref[...] = dot(gathered(0), w_ref[...], 1, 0).astype(bf16)
    keep_ref[...] = dot(gathered(half), w_ref[...], 1, 0)


def local_backward_body(heads, block, q_ref, k_ref, v_ref, g_ref, mem_ref, beta_ref, gq_ref, gk_ref, gv_ref):
    blocks = q_ref.shape[0] // block
    for h in range(heads):
        g = gate(beta_ref, h)
        kt = k_ref[:, cols(h)].T
        gk = [None] * blocks
        gv = [None] * blocks

        def add(acc, i, x):
            acc[i] = x if acc[i] is None else acc[i] + x

        gq = []
        for j in range(blocks):
            q, parts = probs_parts(q_ref, k_ref, h, j, block)
            gl = ((1.0 - g) * g_ref[j * block : (j + 1) * block, cols(h)].astype(f32)).astype(bf16)
            gps = [dot(v_ref[i * block : (i + 1) * block, cols(h)], gl, 1, 1) for i in range(j + 1)]
            delta = sum(jnp.sum(p * gp, 0, keepdims=True) for p, gp in zip(parts, gps))
            acc = None
            for i, (p, gp) in enumerate(zip(parts, gps)):
                gs = (p * (gp - delta) * SCALE).astype(bf16)
                add(gk, i, dot(gs, q, 1, 0))
                add(gv, i, dot(p.astype(bf16), gl, 1, 0))
                t = dot(kt[:, i * block : (i + 1) * block], gs, 1, 0)
                acc = t if acc is None else acc + t
            gq.append(acc.T)
        for i in range(blocks):
            gk_ref[i * block : (i + 1) * block, cols(h)] = gk[i]
            gv_ref[i * block : (i + 1) * block, cols(h)] = gv[i]
        qx = q_ref[:, cols(h)].astype(f32)
        qf = feat(qx)
        mem_out, r, mh, ml, msum = read_memory(qf, mem_ref, heads, h)
        gmem = g * g_ref[:, cols(h)].astype(f32)
        nh, nl = split(gmem * r)
        gden = -jnp.sum(gmem * mem_out, 1, keepdims=True) * r
        gqf = dot(nh, mh, 1, 1) + dot(nl, mh, 1, 1) + dot(nh, ml, 1, 1) + gden * msum
        gq_ref[:, cols(h)] = (jnp.concatenate(gq, 0) + gqf * slope(qx)).astype(bf16)


def final_body(heads, k_ref, v_ref, mem_ref, kl_ref, vl_ref, gk_ref, gv_ref):
    for h in range(heads):
        kx = k_ref[:, cols(h)].astype(f32)
        kh, klo = split(feat(kx))
        mh, ml = split(mem_ref[cols(h), :])
        msum = mem_ref[heads * HD + h : heads * HD + h + 1, :]
        v = v_ref[:, cols(h)]
        gkf = dot(v, mh, 1, 1) + dot(v, ml, 1, 1) + msum
        gk_ref[:, cols(h)] = (kl_ref[:, cols(h)] + gkf * slope(kx)).astype(bf16)
        vm = dot(kh, mh, 1, 0) + dot(klo, mh, 1, 0) + dot(kh, ml, 1, 0)
        gv_ref[:, cols(h)] = (vl_ref[:, cols(h)] + vm).astype(bf16)


def swap(x, axis, bit):
    count = lax.axis_size(axis)
    return lax.ppermute(x, axis, [(i, i ^ bit) for i in range(count)])


def scan(own, axis, backward):
    count = lax.axis_size(axis)
    place = lax.axis_index(axis)
    total = own
    state = jnp.zeros(own.shape, f32)
    bit = 1
    while bit < count:
        other = swap(total.astype(bf16), axis, bit).astype(f32)
        upper = (place & bit) != 0
        take = jnp.logical_not(upper) if backward else upper
        state = state + jnp.where(take, other, 0.0)
        total = total.astype(f32) + other
        bit *= 2
    return state


def reverse_bits(value, count):
    out = 0
    bit = 1
    while bit < count:
        out = out * 2 + (1 if value & bit else 0)
        bit *= 2
    return out


def local(query, keys, values, beta, out_weight, cotangent):
    length, width = query.shape
    heads = width // HD
    model = out_weight.shape[1]
    tp = lax.axis_size("tp")
    place = lax.axis_index("tp")
    block = min(256, length)
    packed = (heads * HD + PAD, HD)

    bit = tp // 2
    pieces = [cotangent]
    while bit:
        pieces = pieces + [swap(p, "tp", bit) for p in pieces]
        bit //= 2
    gather_places = jnp.stack([place ^ reverse_bits(i, tp) for i in range(tp)]).astype(jnp.int32)
    scatter_places = jnp.stack([place ^ reverse_bits(tp - 1 - i, tp) for i in range(tp)]).astype(jnp.int32)

    own = call(
        functools.partial(own_memory_body, heads), [(packed, bf16)], [VM, VM], name="own_memory"
    )(keys, values)[0]
    memory = scan(own, "seq", False)
    local_out = call(
        functools.partial(local_forward_body, heads, block),
        [((length, width), f32)],
        [VM, VM, VM],
        name="local_forward",
    )(query, keys, values)[0]
    grad = call(
        functools.partial(grad_mixed_body, tp),
        [((length, width), bf16)],
        [SM] + [VM] * (tp + 1),
        scratch=[pltpu.VMEM((length, model), bf16)],
        name="grad_mixed",
    )(gather_places, *pieces, out_weight)[0]
    memory_grad = call(
        functools.partial(memory_grad_body, heads),
        [(packed, bf16)],
        [VM, VM, VM, SM],
        name="memory_grad",
    )(query, memory, grad, beta)[0]
    later = scan(memory_grad, "seq", True)
    part = length // tp
    send, keep = call(
        functools.partial(output_body, heads, tp),
        [((length // 2, model), bf16), ((length // 2, model), f32)],
        [SM, VM, VM, VM, SM, VM],
        scratch=[pltpu.VMEM((length, width), bf16)],
        name="output",
    )(scatter_places, query, memory, local_out, beta, out_weight)
    bit = 1
    while bit < tp:
        total = keep + swap(send, "tp", bit).astype(f32)
        bit *= 2
        if bit < tp:
            half = total.shape[0] // 2
            send, keep = total[:half].astype(bf16), total[half:]
    output = total.astype(bf16)
    grad_query, keys_local, values_local = call(
        functools.partial(local_backward_body, heads, block),
        [((length, width), bf16), ((length, width), f32), ((length, width), f32)],
        [VM, VM, VM, VM, VM, SM],
        name="local_backward",
    )(query, keys, values, grad, memory, beta)
    grad_keys, grad_values = call(
        functools.partial(final_body, heads),
        [((length, width), bf16), ((length, width), bf16)],
        [VM, VM, VM, VM, VM],
        name="final",
    )(keys, values, later, keys_local, values_local)
    return (output, grad_query, grad_keys, grad_values)


def solution(mesh):
    in_specs = (
        P("seq", "tp"),
        P("seq", "tp"),
        P("seq", "tp"),
        P("tp"),
        P("tp", None),
        P(("seq", "tp"), None),
    )
    out_specs = (P(("seq", "tp"), None), P("seq", "tp"), P("seq", "tp"), P("seq", "tp"))
    return jax.shard_map(local, mesh=mesh, in_specs=in_specs, out_specs=out_specs, check_vma=False)
```

```python
import functools

import jax
import jax.numpy as jnp
from jax import lax
from jax.experimental import pallas as pl
from jax.experimental.pallas import tpu as pltpu
from jax.sharding import PartitionSpec as P


HD = 128
PAD = 16
SCALE = HD ** (-0.5)

f32 = jnp.float32
bf16 = jnp.bfloat16

VM = pl.BlockSpec(memory_space=pltpu.VMEM)


def dot(a, b, ca, cb):
    return lax.dot_general(a, b, (((ca,), (cb,)), ((), ())), preferred_element_type=f32)


def split(x):
    hi = x.astype(bf16)
    return hi, (x - hi.astype(f32)).astype(bf16)


def feat(x):
    return jnp.where(x > 0, x + 1.0, jnp.exp(jnp.minimum(x, 0.0)))


def slope(x):
    return jnp.where(x > 0, 1.0, jnp.exp(jnp.minimum(x, 0.0)))


def cols(h):
    return slice(h * HD, (h + 1) * HD)


def call(body, outs, specs, out_specs=None, scratch=(), flops=1 << 28, vmem=24, alias=None):
    if out_specs is None:
        out_specs = [VM] * len(outs)
    return pl.pallas_call(
        body,
        out_shape=[jax.ShapeDtypeStruct(s, d) for s, d in outs],
        in_specs=specs,
        out_specs=out_specs,
        scratch_shapes=list(scratch),
        input_output_aliases=alias or {},
        compiler_params=pltpu.CompilerParams(vmem_limit_bytes=vmem << 20),
        cost_estimate=pl.CostEstimate(flops=flops, transcendentals=0, bytes_accessed=1 << 20),
    )


def pad_rows(rows):
    return jnp.concatenate(rows + [jnp.zeros((PAD - len(rows), HD), f32)], 0).astype(bf16)


def own_memory_body(heads, k_hbm, v_hbm, q_hbm, beta_hbm, o_ref, k_ref, v_ref, q_ref, gate_ref, beta_ref, sems, beta_sem):
    beta_copy = pltpu.make_async_copy(beta_hbm, beta_ref, beta_sem)
    pairs = ((k_hbm, k_ref), (v_hbm, v_ref), (q_hbm, q_ref))
    copies = [
        [pltpu.make_async_copy(a.at[:, cols(h)], b.at[:, cols(h)], sems.at[i, h]) for i, (a, b) in enumerate(pairs)]
        for h in range(heads)
    ]
    for h in range(heads):
        copies[h][0].start()
        copies[h][1].start()
    beta_copy.start()
    for h in range(heads):
        copies[h][2].start()
    rows = []
    for h in range(heads):
        copies[h][0].wait()
        copies[h][1].wait()
        kf = feat(k_ref[:, cols(h)].astype(f32))
        hi, lo = split(kf)
        v = v_ref[:, cols(h)]
        o_ref[cols(h), :] = (dot(hi, v, 0, 0) + dot(lo, v, 0, 0)).astype(bf16)
        rows.append(jnp.sum(kf, 0, keepdims=True))
    o_ref[heads * HD :, :] = pad_rows(rows)
    beta_copy.wait()
    for h in range(heads):
        gate_ref[h : h + 1, :] = jax.nn.sigmoid(jnp.full((1, HD), beta_ref[h], f32))
    for h in range(heads):
        copies[h][2].wait()


def add_body(*refs):
    total = refs[0][...].astype(f32)
    for ref in refs[1:-1]:
        total = total + ref[...].astype(f32)
    refs[-1][...] = total.astype(bf16)


def scan_state(refs, backward, rows):
    place = lax.axis_index("seq")
    state = None
    for i, ref in enumerate(refs):
        upper = (place // (1 << i)) % 2
        take = (1 - upper if backward else upper).astype(f32)
        x = ref[rows, :].astype(f32) * take
        state = x if state is None else state + x
    return state


def read_memory(qf, mem_ref, heads, h):
    qh, ql = split(qf)
    mh, ml = split(mem_ref[cols(h), :])
    msum = mem_ref[heads * HD + h : heads * HD + h + 1, :]
    numer = dot(qh, mh, 1, 0) + dot(ql, mh, 1, 0) + dot(qh, ml, 1, 0)
    denom = jnp.sum(qf * msum, 1, keepdims=True) + 1.0
    r = 1.0 / denom
    return numer * r, r, mh, ml, msum


def probs_parts(q_ref, k_ref, h, j, block):
    q = q_ref[j * block : (j + 1) * block, cols(h)]
    parts = []
    for i in range(j + 1):
        k = k_ref[i * block : (i + 1) * block, cols(h)]
        s = dot(k, q, 1, 1) * SCALE
        if i == j:
            shape = (block, block)
            keep = lax.broadcasted_iota(jnp.int32, shape, 0) <= lax.broadcasted_iota(jnp.int32, shape, 1)
            s = jnp.where(keep, s, -jnp.inf)
        parts.append(s)
    top = functools.reduce(jnp.maximum, [jnp.max(s, 0, keepdims=True) for s in parts])
    parts = [jnp.exp(s - top) for s in parts]
    r = 1.0 / sum(jnp.sum(e, 0, keepdims=True) for e in parts)
    return q, [e * r for e in parts]


def local_forward_body(heads, block, q_ref, k_ref, v_ref, o_ref):
    for h in range(heads):
        vt = v_ref[:, cols(h)].T
        for j in range(q_ref.shape[0] // block):
            _, parts = probs_parts(q_ref, k_ref, h, j, block)
            acc = sum(
                dot(vt[:, i * block : (i + 1) * block], p.astype(bf16), 1, 0) for i, p in enumerate(parts)
            )
            o_ref[j * block : (j + 1) * block, cols(h)] = acc.T


def grad_mixed_body(*refs):
    pieces, w_ref, o_ref = refs[:-2], refs[-2], refs[-1]
    x = jnp.concatenate([p[...] for p in pieces], 0)
    o_ref[...] = dot(x, w_ref[...], 1, 1).astype(bf16)


def memory_grad_body(heads, count, order, *refs):
    grads, q_ref, gate_ref = refs[: len(order)], refs[len(order)], refs[len(order) + 1]
    mem_ref = refs[len(order) + 2]
    o_ref, g_ref = refs[-2:]
    place = lax.axis_index("tp")
    for grad, masks in zip(grads, order):
        rows = grad.shape[0] // len(masks)
        for i, m in enumerate(masks):
            spot = pl.multiple_of(flipped(place, m, count) * rows, rows)
            g_ref[pl.ds(spot, rows), :] = grad[i * rows : (i + 1) * rows, :]
    rows = []
    for h in range(heads):
        qf = feat(q_ref[:, cols(h)].astype(f32))
        mem_out, r, _, _, _ = read_memory(qf, mem_ref, heads, h)
        gmem = gate_ref[h : h + 1, :] * g_ref[:, cols(h)].astype(f32)
        nh, nl = split(gmem * r)
        gden = -jnp.sum(gmem * mem_out, 1, keepdims=True) * r
        qh, ql = split(qf)
        o_ref[cols(h), :] = (dot(qh, nh, 0, 0) + dot(ql, nh, 0, 0) + dot(qh, nl, 0, 0)).astype(bf16)
        rows.append(jnp.sum(gden * qf, 0, keepdims=True))
    o_ref[heads * HD :, :] = pad_rows(rows)


def flipped(place, mask, count):
    out = 0
    bit = 1
    while bit < count:
        own = (place // bit) % 2
        out = out + bit * ((1 - own) if mask & bit else own)
        bit *= 2
    return out


def mixed_rows(heads, count, masks, q_ref, mem_ref, lo_ref, gate_ref, mix_ref):
    place = lax.axis_index("tp")
    rows = q_ref.shape[0] // count
    for i, m in enumerate(masks):
        spot = pl.multiple_of(flipped(place, m, count) * rows, rows)
        for h in range(heads):
            qf = feat(q_ref[pl.ds(spot, rows), cols(h)].astype(f32))
            mem_out = read_memory(qf, mem_ref, heads, h)[0]
            g = gate_ref[h : h + 1, :]
            x = g * mem_out + (1.0 - g) * lo_ref[pl.ds(spot, rows), cols(h)]
            mix_ref[i * rows : (i + 1) * rows, cols(h)] = x.astype(bf16)


def output_send_body(heads, count, masks, steps, q_ref, lo_ref, gate_ref, w_ref, *refs):
    recvs, (mem_ref, send_ref, mix_ref) = refs[:steps], refs[steps:]
    mem_ref[...] = scan_state(recvs, False, slice(None))
    mixed_rows(heads, count, masks, q_ref, mem_ref, lo_ref, gate_ref, mix_ref)
    send_ref[...] = dot(mix_ref[...], w_ref[...], 1, 0).astype(bf16)


def output_keep_body(heads, count, masks, q_ref, mem_ref, lo_ref, gate_ref, w_ref, recv_ref, send_ref, keep_ref, mix_ref):
    mixed_rows(heads, count, masks, q_ref, mem_ref, lo_ref, gate_ref, mix_ref)
    total = dot(mix_ref[...], w_ref[...], 1, 0) + recv_ref[...].astype(f32)
    half = send_ref.shape[0]
    send_ref[...] = total[:half].astype(bf16)
    keep_ref[...] = total[half:]


def output_done_body(keep_ref, recv_ref, o_ref):
    o_ref[...] = (keep_ref[...] + recv_ref[...].astype(f32)).astype(bf16)


def local_backward_body(
    heads, group, block, q_ref, k_ref, v_ref, g_ref, mem_ref, gate_ref, *refs
):
    gq_hbm, gk_ref, gv_ref, gq_ref, sems = refs[-5:]
    blocks = q_ref.shape[0] // block
    copies = []
    for n, h in enumerate(group):
        g = gate_ref[h : h + 1, :]
        kt = k_ref[:, cols(h)].T
        gk = [None] * blocks
        gv = [None] * blocks

        def add(acc, i, x):
            acc[i] = x if acc[i] is None else acc[i] + x

        gq = []
        for j in range(blocks):
            q, parts = probs_parts(q_ref, k_ref, h, j, block)
            gl = ((1.0 - g) * g_ref[j * block : (j + 1) * block, cols(h)].astype(f32)).astype(bf16)
            gps = [dot(v_ref[i * block : (i + 1) * block, cols(h)], gl, 1, 1) for i in range(j + 1)]
            delta = sum(jnp.sum(p * gp, 0, keepdims=True) for p, gp in zip(parts, gps))
            acc = None
            for i, (p, gp) in enumerate(zip(parts, gps)):
                gs = (p * (gp - delta) * SCALE).astype(bf16)
                add(gk, i, dot(gs, q, 1, 0))
                add(gv, i, dot(p.astype(bf16), gl, 1, 0))
                t = dot(kt[:, i * block : (i + 1) * block], gs, 1, 0)
                acc = t if acc is None else acc + t
            gq.append(acc.T)
        for i in range(blocks):
            gk_ref[i * block : (i + 1) * block, cols(n)] = gk[i]
            gv_ref[i * block : (i + 1) * block, cols(n)] = gv[i]
        qx = q_ref[:, cols(h)].astype(f32)
        qf = feat(qx)
        mem_out, r, mh, ml, msum = read_memory(qf, mem_ref, heads, h)
        gmem = g * g_ref[:, cols(h)].astype(f32)
        nh, nl = split(gmem * r)
        gden = -jnp.sum(gmem * mem_out, 1, keepdims=True) * r
        gqf = dot(nh, mh, 1, 1) + dot(nl, mh, 1, 1) + dot(nh, ml, 1, 1) + gden * msum
        gq_ref[:, cols(n)] = (jnp.concatenate(gq, 0) + gqf * slope(qx)).astype(bf16)
        copy = pltpu.make_async_copy(gq_ref.at[:, cols(n)], gq_hbm.at[:, cols(h)], sems.at[n])
        copy.start()
        copies.append(copy)
    for copy in copies:
        copy.wait()


def final_body(heads, groups, steps, *refs):
    k_ref, v_ref = refs[:2]
    recvs = refs[2 : 2 + steps]
    locals_ = refs[2 + steps : 2 + steps + 2 * len(groups)]
    gk_hbm, gv_hbm, gk_ref, gv_ref, sems = refs[-5:]
    sums = scan_state(recvs, True, slice(heads * HD, heads * HD + PAD))
    copies = []
    for n, group in enumerate(groups):
        kl_ref, vl_ref = locals_[2 * n : 2 * n + 2]
        for i, h in enumerate(group):
            kx = k_ref[:, cols(h)].astype(f32)
            kh, klo = split(feat(kx))
            mh, ml = split(scan_state(recvs, True, cols(h)))
            v = v_ref[:, cols(h)]
            gkf = dot(v, mh, 1, 1) + dot(v, ml, 1, 1) + sums[h : h + 1, :]
            gk_ref[:, cols(h)] = (kl_ref[:, cols(i)] + gkf * slope(kx)).astype(bf16)
            copies.append(pltpu.make_async_copy(gk_ref.at[:, cols(h)], gk_hbm.at[:, cols(h)], sems.at[0, h]))
            copies[-1].start()
            vm = dot(kh, mh, 1, 0) + dot(klo, mh, 1, 0) + dot(kh, ml, 1, 0)
            gv_ref[:, cols(h)] = (vl_ref[:, cols(i)] + vm).astype(bf16)
            copies.append(pltpu.make_async_copy(gv_ref.at[:, cols(h)], gv_hbm.at[:, cols(h)], sems.at[1, h]))
            copies[-1].start()
    for copy in copies:
        copy.wait()


def swap(x, axis, bit):
    count = lax.axis_size(axis)
    return lax.ppermute(x, axis, [(i, i ^ bit) for i in range(count)])


def scan(own, axis):
    count = lax.axis_size(axis)
    recvs = []
    send = own
    bit = 1
    while bit < count:
        step = len(recvs)
        if step:
            specs = [VM] * (step + 1)
            send = call(add_body, [(own.shape, bf16)], specs, flops=1 << 20)(own, *recvs)[0]
        recvs.append(swap(send, axis, bit))
        bit *= 2
    return recvs


def reverse_bits(value, count):
    out = 0
    bit = 1
    while bit < count:
        out = out * 2 + (1 if value & bit else 0)
        bit *= 2
    return out


def local(query, keys, values, beta, out_weight, cotangent):
    length, width = query.shape
    heads = width // HD
    model = out_weight.shape[1]
    tp = lax.axis_size("tp")
    block = min(256, length)
    packed = (heads * HD + PAD, HD)
    hbm = pl.BlockSpec(memory_space=pltpu.HBM)
    full = (length, width)

    own, keys, values, query, gates = call(
        functools.partial(own_memory_body, heads),
        [(packed, bf16), (full, bf16), (full, bf16), (full, bf16), ((8, HD), f32)],
        [hbm] * 4,
        scratch=[pltpu.SMEM((heads,), f32), pltpu.SemaphoreType.DMA((3, heads)), pltpu.SemaphoreType.DMA],
    )(*[pltpu.with_memory_space_constraint(x, pltpu.HBM) for x in (keys, values, query, beta)])
    fwd = scan(own, "seq")
    steps = len(fwd)

    held = {0: cotangent}
    first, second = [0], []
    if tp > 1:
        held[1] = swap(cotangent, "tp", 1)
        first = [0, 1]
    bit = 2
    far = [0]
    while bit < tp:
        for m in list(far):
            held[m | bit] = swap(held[m], "tp", bit)
            far.append(m | bit)
        bit *= 2
    for m in far[1:]:
        held[m | 1] = swap(held[m], "tp", 1)
        second += [m, m | 1]
    order = [first] + ([second] if second else [])

    local_out = call(
        functools.partial(local_forward_body, heads, block), [(full, f32)], [VM, VM, VM]
    )(query, keys, values)[0]

    grads = []
    for masks in order:
        rows = cotangent.shape[0] * len(masks)
        grads.append(
            call(
                grad_mixed_body, [((rows, width), bf16)], [VM] * (len(masks) + 1)
            )(*[held[m] for m in masks], out_weight)[0]
        )

    places = [reverse_bits(tp - 1 - i, tp) for i in range(tp)]
    half = tp // 2
    memory, send = call(
        functools.partial(output_send_body, heads, tp, places[:half], steps),
        [(packed, f32), ((length // 2, model), bf16)],
        [VM] * (4 + steps),
        scratch=[pltpu.VMEM((length // 2, width), bf16)],
    )(query, local_out, gates, out_weight, *fwd)
    recv = swap(send, "tp", 1)

    memory_grad, grad = call(
        functools.partial(memory_grad_body, heads, tp, order), [(packed, bf16), (full, bf16)], [VM] * (len(order) + 3)
    )(*grads, query, gates, memory)
    bwd = scan(memory_grad, "seq")

    quarter = length // 4
    send, keep = call(
        functools.partial(output_keep_body, heads, tp, places[half:]),
        [((quarter, model), bf16), ((quarter, model), f32)],
        [VM] * 6,
        scratch=[pltpu.VMEM((length // 2, width), bf16)],
    )(query, memory, local_out, gates, out_weight, recv)
    bit = 2
    while 2 * bit < tp:
        total = keep + swap(send, "tp", bit).astype(f32)
        part = total.shape[0] // 2
        send, keep = total[:part].astype(bf16), total[part:]
        bit *= 2
    recv = swap(send, "tp", bit)
    output = call(output_done_body, [((length // tp, model), bf16)], [VM, VM], flops=1 << 20)(keep, recv)[0]

    cut = max(1, heads // 2)
    groups = [list(range(i, min(heads, i + cut))) for i in range(0, heads, cut)]
    grad_query = None
    locals_ = []
    for group in groups:
        part = (length, len(group) * HD)
        args = [query, keys, values, grad, memory, gates]
        specs = [VM] * 6
        alias = None
        if grad_query is not None:
            args.append(grad_query)
            specs.append(hbm)
            alias = {6: 0}
        grad_query, kl, vl = call(
            functools.partial(local_backward_body, heads, group, block),
            [(full, bf16), (part, f32), (part, f32)],
            specs,
            out_specs=[hbm, VM, VM],
            scratch=[pltpu.VMEM(part, bf16), pltpu.SemaphoreType.DMA((len(group),))],
            alias=alias,
        )(*args)
        locals_ += [kl, vl]
    grad_keys, grad_values = call(
        functools.partial(final_body, heads, groups, steps),
        [(full, bf16), (full, bf16)],
        [VM] * (2 + steps + len(locals_)),
        out_specs=[hbm, hbm],
        scratch=[pltpu.VMEM(full, bf16), pltpu.VMEM(full, bf16), pltpu.SemaphoreType.DMA((2, heads))],
    )(keys, values, *bwd, *locals_)
    return (output, grad_query, grad_keys, grad_values)


def solution(mesh):
    in_specs = (
        P("seq", "tp"),
        P("seq", "tp"),
        P("seq", "tp"),
        P("tp"),
        P("tp", None),
        P(("seq", "tp"), None),
    )
    out_specs = (P(("seq", "tp"), None), P("seq", "tp"), P("seq", "tp"), P("seq", "tp"))

    return jax.shard_map(local, mesh=mesh, in_specs=in_specs, out_specs=out_specs, check_vma=False)
```

```python
import functools

import jax
import jax.numpy as jnp
from jax import lax
from jax.experimental import pallas as pl
from jax.experimental.pallas import tpu as pltpu
from jax.sharding import PartitionSpec as P


HD = 128
PAD = 16
SCALE = HD ** (-0.5)

f32 = jnp.float32
bf16 = jnp.bfloat16

VM = pl.BlockSpec(memory_space=pltpu.VMEM)


def dot(a, b, ca, cb):
    return lax.dot_general(a, b, (((ca,), (cb,)), ((), ())), preferred_element_type=f32)


def split(x):
    hi = x.astype(bf16)
    return hi, (x - hi.astype(f32)).astype(bf16)


def side(a, b):
    return jnp.concatenate([a, b], 1)


def halves(y):
    return y[:, : y.shape[1] // 2] + y[:, y.shape[1] // 2 :]


def twofold(x, m, transposed=False):
    mh, ml = split(m)
    both = jnp.concatenate([mh, ml], 0) if transposed else side(mh, ml)
    if transposed:
        return halves(dot(side(*split(x)), side(both, both), 1, 1))
    return halves(dot(side(*split(x)), jnp.concatenate([both, both], 0), 1, 0))


def feat(x):
    return jnp.where(x > 0, x + 1.0, jnp.exp(jnp.minimum(x, 0.0)))


def slope(x):
    return jnp.where(x > 0, 1.0, jnp.exp(jnp.minimum(x, 0.0)))


def cols(h):
    return slice(h * HD, (h + 1) * HD)


def call(body, outs, specs, out_specs=None, scratch=(), flops=1 << 28, vmem=24, alias=None):
    if out_specs is None:
        out_specs = [VM] * len(outs)
    return pl.pallas_call(
        body,
        out_shape=[jax.ShapeDtypeStruct(s, d) for s, d in outs],
        in_specs=specs,
        out_specs=out_specs,
        scratch_shapes=list(scratch),
        input_output_aliases=alias or {},
        compiler_params=pltpu.CompilerParams(vmem_limit_bytes=vmem << 20),
        cost_estimate=pl.CostEstimate(flops=flops, transcendentals=0, bytes_accessed=1 << 20),
    )


def pad_rows(rows):
    return jnp.concatenate(rows + [jnp.zeros((PAD - len(rows), HD), f32)], 0).astype(bf16)


def rows_of(h):
    return slice(PAD + h * HD, PAD + (h + 1) * HD)


def memory_of(mem_ref, h):
    return mem_ref[rows_of(h), :], mem_ref[h : h + 1, :]


def own_memory_body(heads, k_hbm, v_hbm, o_ref, k_ref, v_ref, sems):
    part = k_ref.shape[0] // heads
    blocks = [slice(i * part, (i + 1) * part) for i in range(heads)]
    copies = [
        [pltpu.make_async_copy(a.at[rows], b.at[rows], sems.at[i, n]) for i, (a, b) in enumerate(((k_hbm, k_ref), (v_hbm, v_ref)))]
        for n, rows in enumerate(blocks)
    ]
    for pair in copies:
        for copy in pair:
            copy.start()
    both = [None] * heads
    sums = [None] * heads
    for rows, pair in zip(blocks, copies):
        for copy in pair:
            copy.wait()
        for h in range(heads):
            kf = feat(k_ref[rows, cols(h)].astype(f32))
            x = dot(side(*split(kf)), v_ref[rows, cols(h)], 0, 0)
            y = jnp.sum(kf, 0, keepdims=True)
            both[h] = x if both[h] is None else both[h] + x
            sums[h] = y if sums[h] is None else sums[h] + y
    for h in range(heads):
        o_ref[rows_of(h), :] = (both[h][:HD] + both[h][HD:]).astype(bf16)
    o_ref[:PAD, :] = pad_rows(sums)


def load_query_body(heads, q_hbm, beta_hbm, q_ref, qt_ref, gate_ref, beta_ref, sems):
    rows = q_ref.shape[0] // heads
    beta_copy = pltpu.make_async_copy(beta_hbm, beta_ref, sems.at[heads])
    beta_copy.start()
    parts = [pl.ds(i * rows, rows) for i in range(heads)]
    copies = [pltpu.make_async_copy(q_hbm.at[p], q_ref.at[p], sems.at[i]) for i, p in enumerate(parts)]
    for copy in copies:
        copy.start()
    beta_copy.wait()
    for h in range(heads):
        gate_ref[h : h + 1, :] = jax.nn.sigmoid(jnp.full((1, HD), beta_ref[h], f32))
    for copy in copies:
        copy.wait()
    for h in range(heads):
        both = side(*split(feat(q_ref[:, cols(h)].astype(f32))))
        qt_ref[2 * h * HD : 2 * (h + 1) * HD, :] = both.T


def add_body(count, *refs):
    total = refs[0][...].astype(f32)
    for ref in refs[1:count]:
        total = total + ref[...].astype(f32)
    start = 0
    for out in refs[count:]:
        out[...] = total[start : start + out.shape[0]].astype(bf16)
        start += out.shape[0]


def scan_state(backward, refs, rows):
    place = lax.axis_index("seq")
    cut = refs[-2].shape[0] if refs[-1] is not None else None
    state = None
    for i, ref in enumerate(refs[:-1]):
        upper = (place // (1 << i)) % 2
        take = (1 - upper if backward else upper).astype(f32)
        part = rows
        if i == len(refs) - 2 and cut is not None and rows.start >= cut:
            ref, part = refs[-1], slice(rows.start - cut, rows.stop - cut)
        x = ref[part, :].astype(f32) * take
        state = x if state is None else state + x
    return state


def read_memory(qf, matrix, msum):
    numer = twofold(qf, matrix)
    r = 1.0 / (jnp.sum(qf * msum, 1, keepdims=True) + 1.0)
    return numer * r, r


def probs_parts(q_ref, k_ref, h, j, block):
    q = q_ref[j * block : (j + 1) * block, cols(h)]
    parts = []
    for i in range(j + 1):
        k = k_ref[i * block : (i + 1) * block, cols(h)]
        s = dot(k, q, 1, 1) * SCALE
        if i == j:
            shape = (block, block)
            keep = lax.broadcasted_iota(jnp.int32, shape, 0) <= lax.broadcasted_iota(jnp.int32, shape, 1)
            s = jnp.where(keep, s, -jnp.inf)
        parts.append(s)
    top = functools.reduce(jnp.maximum, [jnp.max(s, 0, keepdims=True) for s in parts])
    parts = [jnp.exp(s - top) for s in parts]
    r = 1.0 / sum(jnp.sum(e, 0, keepdims=True) for e in parts)
    return q, [e * r for e in parts]


def local_forward_body(heads, block, q_ref, k_ref, v_ref, o_ref):
    for h in range(heads):
        vt = v_ref[:, cols(h)].T
        for j in range(q_ref.shape[0] // block):
            _, parts = probs_parts(q_ref, k_ref, h, j, block)
            acc = sum(
                dot(vt[:, i * block : (i + 1) * block], p.astype(bf16), 1, 0) for i, p in enumerate(parts)
            )
            o_ref[j * block : (j + 1) * block, cols(h)] = acc.T


def grad_mixed_body(*refs):
    pieces, w_ref, o_ref = refs[:-2], refs[-2], refs[-1]
    x = jnp.concatenate([p[...] for p in pieces], 0)
    o_ref[...] = dot(x, w_ref[...], 1, 1).astype(bf16)


def gather_grad(count, order, grads, g_ref):
    place = lax.axis_index("tp")
    for grad, masks in zip(grads, order):
        rows = grad.shape[0] // len(masks)
        for i, m in enumerate(masks):
            spot = pl.multiple_of(flipped(place, m, count) * rows, rows)
            g_ref[pl.ds(spot, rows), :] = grad[i * rows : (i + 1) * rows, :]


def segment_memory_grad(h, q_ref, qt_ref, g_ref, gate_ref, matrix, msum):
    qf = feat(q_ref[:, cols(h)].astype(f32))
    mem_out, r = read_memory(qf, matrix, msum)
    gmem = gate_ref[h : h + 1, :] * g_ref[:, cols(h)].astype(f32)
    gden = -jnp.sum(gmem * mem_out, 1, keepdims=True) * r
    both = halves(dot(qt_ref[2 * h * HD : 2 * (h + 1) * HD, :], side(*split(gmem * r)), 1, 0))
    return (both[:HD] + both[HD:]).astype(bf16), jnp.sum(gden * qf, 0, keepdims=True)


def memory_grad_first_body(group, count, order, steps, *refs):
    grads, (q_ref, qt_ref, gate_ref) = refs[: len(order)], refs[len(order) : len(order) + 3]
    recvs = refs[len(order) + 3 : len(order) + 3 + steps] + (None,)
    o_ref, g_ref = refs[-2:]
    gather_grad(count, order, grads, g_ref)
    sums = scan_state(False, recvs, slice(0, PAD))
    rows = []
    for h in group:
        matrix = scan_state(False, recvs, rows_of(h))
        o_ref[rows_of(h), :], row = segment_memory_grad(h, q_ref, qt_ref, g_ref, gate_ref, matrix, sums[h : h + 1, :])
        rows.append(row)
    o_ref[:PAD, :] = jnp.concatenate(rows + [jnp.zeros((PAD - len(rows), HD), f32)], 0).astype(bf16)


def memory_grad_second_body(first, group, first_ref, q_ref, qt_ref, gate_ref, g_ref, mem_ref, o_ref):
    cut = first_ref.shape[0]
    o_ref[:cut, :] = first_ref[...]
    rows = []
    for h in group:
        o_ref[rows_of(h), :], row = segment_memory_grad(h, q_ref, qt_ref, g_ref, gate_ref, *memory_of(mem_ref, h))
        rows.append(row)
    head = first_ref[:PAD, :].astype(f32)
    tail = [jnp.zeros((PAD - first - len(rows), HD), f32)]
    o_ref[:PAD, :] = jnp.concatenate([head[:first]] + rows + tail, 0).astype(bf16)


def flipped(place, mask, count):
    out = 0
    bit = 1
    while bit < count:
        own = (place // bit) % 2
        out = out + bit * ((1 - own) if mask & bit else own)
        bit *= 2
    return out


def mixed_rows(heads, count, masks, q_ref, mem_ref, lo_ref, gate_ref, mix_ref):
    place = lax.axis_index("tp")
    rows = q_ref.shape[0] // count
    for i, m in enumerate(masks):
        spot = pl.multiple_of(flipped(place, m, count) * rows, rows)
        for h in range(heads):
            qf = feat(q_ref[pl.ds(spot, rows), cols(h)].astype(f32))
            mem_out = read_memory(qf, *memory_of(mem_ref, h))[0]
            g = gate_ref[h : h + 1, :]
            x = g * mem_out + (1.0 - g) * lo_ref[pl.ds(spot, rows), cols(h)]
            mix_ref[i * rows : (i + 1) * rows, cols(h)] = x.astype(bf16)


def output_send_body(heads, count, masks, steps, q_ref, lo_ref, gate_ref, w_ref, *refs):
    recvs, (mem_ref, send_ref, mix_ref) = refs[:steps], refs[steps:]
    cut = recvs[-2].shape[0]
    for rows in (slice(0, cut), slice(cut, mem_ref.shape[0])):
        mem_ref[rows, :] = scan_state(False, recvs, rows)
    mixed_rows(heads, count, masks, q_ref, mem_ref, lo_ref, gate_ref, mix_ref)
    send_ref[...] = dot(mix_ref[...], w_ref[...], 1, 0).astype(bf16)


def output_keep_body(heads, count, masks, q_ref, mem_ref, lo_ref, gate_ref, w_ref, recv_ref, send_ref, keep_ref, mix_ref):
    mixed_rows(heads, count, masks, q_ref, mem_ref, lo_ref, gate_ref, mix_ref)
    total = dot(mix_ref[...], w_ref[...], 1, 0) + recv_ref[...].astype(f32)
    half = send_ref.shape[0]
    send_ref[...] = total[:half].astype(bf16)
    keep_ref[...] = total[half:]


def output_done_body(keep_ref, recv_ref, o_ref):
    o_ref[...] = (keep_ref[...] + recv_ref[...].astype(f32)).astype(bf16)


def local_backward_body(group, block, q_ref, k_ref, v_ref, g_ref, mem_ref, gate_ref, *refs):
    gq_ref, gk_ref, gv_ref = refs
    blocks = q_ref.shape[0] // block
    for n, h in enumerate(group):
        g = gate_ref[h : h + 1, :]
        kt = k_ref[:, cols(h)].T
        gk = [None] * blocks
        gv = [None] * blocks

        def add(acc, i, x):
            acc[i] = x if acc[i] is None else acc[i] + x

        gq = []
        for j in range(blocks):
            q, parts = probs_parts(q_ref, k_ref, h, j, block)
            gl = ((1.0 - g) * g_ref[j * block : (j + 1) * block, cols(h)].astype(f32)).astype(bf16)
            gps = [dot(v_ref[i * block : (i + 1) * block, cols(h)], gl, 1, 1) for i in range(j + 1)]
            delta = sum(jnp.sum(p * gp, 0, keepdims=True) for p, gp in zip(parts, gps))
            acc = None
            for i, (p, gp) in enumerate(zip(parts, gps)):
                gs = (p * (gp - delta) * SCALE).astype(bf16)
                add(gk, i, dot(gs, q, 1, 0))
                add(gv, i, dot(p.astype(bf16), gl, 1, 0))
                t = dot(kt[:, i * block : (i + 1) * block], gs, 1, 0)
                acc = t if acc is None else acc + t
            gq.append(acc.T)
        for i in range(blocks):
            gk_ref[i * block : (i + 1) * block, cols(n)] = gk[i]
            gv_ref[i * block : (i + 1) * block, cols(n)] = gv[i]
        qx = q_ref[:, cols(h)].astype(f32)
        qf = feat(qx)
        matrix, msum = memory_of(mem_ref, h)
        mem_out, r = read_memory(qf, matrix, msum)
        gmem = g * g_ref[:, cols(h)].astype(f32)
        gden = -jnp.sum(gmem * mem_out, 1, keepdims=True) * r
        gqf = twofold(gmem * r, matrix, True) + gden * msum
        gq_ref[:, cols(n)] = (jnp.concatenate(gq, 0) + gqf * slope(qx)).astype(bf16)


def final_body(group, moves, steps, *refs):
    k_ref, v_ref, kl_ref, vl_ref = refs[:4]
    recvs = refs[4 : 4 + steps]
    if group[0] == 0:
        recvs = recvs + (None,)
    gqs = refs[4 + steps : 4 + steps + len(moves)]
    gq_hbm, gk_hbm, gv_hbm, gk_ref, gv_ref, sems, gq_sems = refs[-7:]
    copies = []
    for n, (ref, spots) in enumerate(zip(gqs, moves)):
        copies.append(pltpu.make_async_copy(ref, gq_hbm.at[:, spots], gq_sems.at[n]))
        copies[-1].start()
    for i, h in enumerate(group):
        kx = k_ref[:, cols(h)].astype(f32)
        matrix = scan_state(True, recvs, rows_of(h))
        msum = scan_state(True, recvs, slice(0, PAD))[h : h + 1, :]
        gkf = halves(dot(v_ref[:, cols(h)], jnp.concatenate(split(matrix), 0), 1, 1)) + msum
        gk_ref[:, cols(i)] = (kl_ref[:, cols(i)] + gkf * slope(kx)).astype(bf16)
        copies.append(pltpu.make_async_copy(gk_ref.at[:, cols(i)], gk_hbm.at[:, cols(h)], sems.at[0, i]))
        copies[-1].start()
        gv_ref[:, cols(i)] = (vl_ref[:, cols(i)] + twofold(feat(kx), matrix)).astype(bf16)
        copies.append(pltpu.make_async_copy(gv_ref.at[:, cols(i)], gv_hbm.at[:, cols(h)], sems.at[1, i]))
        copies[-1].start()
    for copy in copies:
        copy.wait()


def swap(x, axis, bit):
    count = lax.axis_size(axis)
    return lax.ppermute(x, axis, [(i, i ^ bit) for i in range(count)])


def scan(own, axis, cut):
    count = lax.axis_size(axis)
    recvs = []
    bit = 1
    while bit < count:
        have = [own] + recvs
        shapes = [own.shape]
        ends = bit * 2 == count
        if ends:
            shapes = [(cut, HD), (own.shape[0] - cut, HD)]
        sends = [own]
        if len(have) > 1 or ends:
            body = functools.partial(add_body, len(have))
            outs = [(shape, bf16) for shape in shapes]
            sends = call(body, outs, [VM] * len(have), flops=1 << 20)(*have)
        for send in sends:
            recvs.append(swap(send, axis, bit))
        bit *= 2
    return recvs


def reverse_bits(value, count):
    out = 0
    bit = 1
    while bit < count:
        out = out * 2 + (1 if value & bit else 0)
        bit *= 2
    return out


def local(query, keys, values, beta, out_weight, cotangent):
    length, width = query.shape
    heads = width // HD
    model = out_weight.shape[1]
    tp = lax.axis_size("tp")
    block = min(256, length)
    packed = (heads * HD + PAD, HD)
    hbm = pl.BlockSpec(memory_space=pltpu.HBM)
    full = (length, width)
    first = -(-heads // 2)
    groups = [list(range(first)), list(range(first, heads))]
    cut = PAD + first * HD

    def in_hbm(*xs):
        return [pltpu.with_memory_space_constraint(x, pltpu.HBM) for x in xs]

    own, keys, values = call(
        functools.partial(own_memory_body, heads),
        [(packed, bf16), (full, bf16), (full, bf16)],
        [hbm] * 2,
        scratch=[pltpu.SemaphoreType.DMA((2, heads))],
    )(*in_hbm(keys, values))
    query, query_t, gates = call(
        functools.partial(load_query_body, heads),
        [(full, bf16), ((2 * width, length), bf16), ((-(-heads // 8) * 8, HD), f32)],
        [hbm] * 2,
        scratch=[pltpu.SMEM((heads,), f32), pltpu.SemaphoreType.DMA((heads + 1,))],
        flops=1 << 16,
    )(*in_hbm(query, beta))
    fwd = scan(own, "seq", cut)

    held = {0: cotangent}
    near, later = [0], []
    if tp > 1:
        held[1] = swap(cotangent, "tp", 1)
        near = [0, 1]
    bit = 2
    far = [0]
    while bit < tp:
        for m in list(far):
            held[m | bit] = swap(held[m], "tp", bit)
            far.append(m | bit)
        bit *= 2
    for m in far[1:]:
        held[m | 1] = swap(held[m], "tp", 1)
        later += [m, m | 1]
    order = [near] + ([later] if later else [])

    local_out = call(
        functools.partial(local_forward_body, heads, block), [(full, f32)], [VM, VM, VM]
    )(query, keys, values)[0]

    grads = []
    for masks in order:
        rows = cotangent.shape[0] * len(masks)
        grads.append(
            call(
                grad_mixed_body, [((rows, width), bf16)], [VM] * (len(masks) + 1)
            )(*[held[m] for m in masks], out_weight)[0]
        )

    places = [reverse_bits(tp - 1 - i, tp) for i in range(tp)]
    half = tp // 2
    steps = len(fwd)
    part, grad = call(
        functools.partial(memory_grad_first_body, groups[0], tp, order, steps - 1),
        [((cut, HD), bf16), (full, bf16)],
        [VM] * (len(order) + 2 + steps),
    )(*grads, query, query_t, gates, *fwd[:-1])
    memory, send = call(
        functools.partial(output_send_body, heads, tp, places[:half], steps),
        [(packed, f32), ((length // 2, model), bf16)],
        [VM] * (4 + steps),
        scratch=[pltpu.VMEM((length // 2, width), bf16)],
    )(query, local_out, gates, out_weight, *fwd)
    recv = swap(send, "tp", 1)
    memory_grad = call(
        functools.partial(memory_grad_second_body, first, groups[1]), [(packed, bf16)], [VM] * 6
    )(part, query, query_t, gates, grad, memory)[0]
    bwd = scan(memory_grad, "seq", cut)

    quarter = length // 4
    send, keep = call(
        functools.partial(output_keep_body, heads, tp, places[half:]),
        [((quarter, model), bf16), ((quarter, model), f32)],
        [VM] * 6,
        scratch=[pltpu.VMEM((length // 2, width), bf16)],
    )(query, memory, local_out, gates, out_weight, recv)
    bit = 2
    while 2 * bit < tp:
        total = keep + swap(send, "tp", bit).astype(f32)
        part = total.shape[0] // 2
        send, keep = total[:part].astype(bf16), total[part:]
        bit *= 2
    recv = swap(send, "tp", bit)
    output = call(
        output_done_body, [((length // tp, model), bf16)], [VM, VM], flops=1 << 20
    )(keep, recv)[0]

    pieces = []
    for group in groups:
        part = (length, len(group) * HD)
        pieces.append(
            call(
                functools.partial(local_backward_body, group, block),
                [(part, bf16), (part, f32), (part, f32)],
                [VM] * 6,
            )(query, keys, values, grad, memory, gates)
        )
    grads_out = None
    for n, group in enumerate(groups):
        recvs = bwd[:-1] if n == 0 else bwd
        args = [keys, values, *pieces[n][1:], *recvs]
        specs = [VM] * len(args)
        moves, alias = [], None
        if n == 0:
            args += [piece[0] for piece in pieces]
            specs += [VM] * len(pieces)
            moves = [slice(g[0] * HD, (g[-1] + 1) * HD) for g in groups]
        else:
            alias = {len(args) + i: i for i in range(3)}
            args += grads_out
            specs += [hbm] * 3
        part = (length, len(group) * HD)
        grads_out = call(
            functools.partial(final_body, group, moves, len(recvs)),
            [(full, bf16)] * 3,
            specs,
            out_specs=[hbm] * 3,
            scratch=[
                pltpu.VMEM(part, bf16),
                pltpu.VMEM(part, bf16),
                pltpu.SemaphoreType.DMA((2, len(group))),
                pltpu.SemaphoreType.DMA((len(groups),)),
            ],
            alias=alias,
        )(*args)
    grad_query, grad_keys, grad_values = grads_out
    return (output, grad_query, grad_keys, grad_values)


def solution(mesh):
    in_specs = (
        P("seq", "tp"),
        P("seq", "tp"),
        P("seq", "tp"),
        P("tp"),
        P("tp", None),
        P(("seq", "tp"), None),
    )
    out_specs = (P(("seq", "tp"), None), P("seq", "tp"), P("seq", "tp"), P("seq", "tp"))

    return jax.shard_map(local, mesh=mesh, in_specs=in_specs, out_specs=out_specs, check_vma=False)
```

```python
import functools

import jax
import jax.numpy as jnp
from jax import lax
from jax.experimental import pallas as pl
from jax.experimental.pallas import tpu as pltpu
from jax.sharding import PartitionSpec as P


HD = 128
PAD = 16
SCALE = HD ** (-0.5)

f32 = jnp.float32
bf16 = jnp.bfloat16

VM = pl.BlockSpec(memory_space=pltpu.VMEM)


def dot(a, b, ca, cb):
    return lax.dot_general(a, b, (((ca,), (cb,)), ((), ())), preferred_element_type=f32)


def split(x):
    hi = x.astype(bf16)
    return hi, (x - hi.astype(f32)).astype(bf16)


def side(a, b):
    return jnp.concatenate([a, b], 1)


def halves(y):
    return y[:, : y.shape[1] // 2] + y[:, y.shape[1] // 2 :]


def twofold(x, m, transposed=False):
    mh, ml = split(m)
    both = jnp.concatenate([mh, ml], 0) if transposed else side(mh, ml)
    if transposed:
        return halves(dot(side(*split(x)), side(both, both), 1, 1))
    return halves(dot(side(*split(x)), jnp.concatenate([both, both], 0), 1, 0))


def feat(x):
    return jnp.where(x > 0, x + 1.0, jnp.exp(jnp.minimum(x, 0.0)))


def slope(x):
    return jnp.where(x > 0, 1.0, jnp.exp(jnp.minimum(x, 0.0)))


def cols(h):
    return slice(h * HD, (h + 1) * HD)


def call(body, outs, specs, out_specs=None, scratch=(), flops=1 << 28, vmem=24, alias=None):
    if out_specs is None:
        out_specs = [VM] * len(outs)
    return pl.pallas_call(
        body,
        out_shape=[jax.ShapeDtypeStruct(s, d) for s, d in outs],
        in_specs=specs,
        out_specs=out_specs,
        scratch_shapes=list(scratch),
        input_output_aliases=alias or {},
        compiler_params=pltpu.CompilerParams(vmem_limit_bytes=vmem << 20),
        cost_estimate=pl.CostEstimate(flops=flops, transcendentals=0, bytes_accessed=1 << 20),
    )


def pad_rows(rows):
    return jnp.concatenate(rows + [jnp.zeros((PAD - len(rows), HD), f32)], 0).astype(bf16)


def rows_of(h):
    return slice(PAD + h * HD, PAD + (h + 1) * HD)


def memory_of(mem_ref, h):
    return mem_ref[rows_of(h), :], mem_ref[h : h + 1, :]


def own_memory_body(heads, k_hbm, v_hbm, o_ref, k_ref, v_ref, sems):
    part = k_ref.shape[0] // heads
    blocks = [slice(i * part, (i + 1) * part) for i in range(heads)]
    copies = [
        [pltpu.make_async_copy(a.at[rows], b.at[rows], sems.at[i, n]) for i, (a, b) in enumerate(((k_hbm, k_ref), (v_hbm, v_ref)))]
        for n, rows in enumerate(blocks)
    ]
    for pair in copies:
        for copy in pair:
            copy.start()
    both = [None] * heads
    sums = [None] * heads
    for rows, pair in zip(blocks, copies):
        for copy in pair:
            copy.wait()
        for h in range(heads):
            kf = feat(k_ref[rows, cols(h)].astype(f32))
            x = dot(side(*split(kf)), v_ref[rows, cols(h)], 0, 0)
            y = jnp.sum(kf, 0, keepdims=True)
            both[h] = x if both[h] is None else both[h] + x
            sums[h] = y if sums[h] is None else sums[h] + y
    for h in range(heads):
        o_ref[rows_of(h), :] = (both[h][:HD] + both[h][HD:]).astype(bf16)
    o_ref[:PAD, :] = pad_rows(sums)


def load_query_body(heads, q_hbm, beta_hbm, q_ref, qt_ref, gate_ref, beta_ref, sems):
    rows = q_ref.shape[0] // heads
    beta_copy = pltpu.make_async_copy(beta_hbm, beta_ref, sems.at[heads])
    beta_copy.start()
    parts = [pl.ds(i * rows, rows) for i in range(heads)]
    copies = [pltpu.make_async_copy(q_hbm.at[p], q_ref.at[p], sems.at[i]) for i, p in enumerate(parts)]
    for copy in copies:
        copy.start()
    beta_copy.wait()
    for h in range(heads):
        gate_ref[h : h + 1, :] = jax.nn.sigmoid(jnp.full((1, HD), beta_ref[h], f32))
    for copy in copies:
        copy.wait()
    for h in range(heads):
        both = side(*split(feat(q_ref[:, cols(h)].astype(f32))))
        qt_ref[2 * h * HD : 2 * (h + 1) * HD, :] = both.T


def add_body(count, *refs):
    total = refs[0][...].astype(f32)
    for ref in refs[1:count]:
        total = total + ref[...].astype(f32)
    start = 0
    for out in refs[count:]:
        out[...] = total[start : start + out.shape[0]].astype(bf16)
        start += out.shape[0]


def scan_state(backward, refs, rows):
    place = lax.axis_index("seq")
    cut = refs[-2].shape[0] if refs[-1] is not None else None
    state = None
    for i, ref in enumerate(refs[:-1]):
        upper = (place // (1 << i)) % 2
        take = (1 - upper if backward else upper).astype(f32)
        part = rows
        if i == len(refs) - 2 and cut is not None and rows.start >= cut:
            ref, part = refs[-1], slice(rows.start - cut, rows.stop - cut)
        x = ref[part, :].astype(f32) * take
        state = x if state is None else state + x
    return state


def read_memory(qf, matrix, msum):
    numer = twofold(qf, matrix)
    r = 1.0 / (jnp.sum(qf * msum, 1, keepdims=True) + 1.0)
    return numer * r, r


def probs_parts(q_ref, k_ref, h, j, block):
    q = q_ref[j * block : (j + 1) * block, cols(h)]
    parts = []
    for i in range(j + 1):
        k = k_ref[i * block : (i + 1) * block, cols(h)]
        s = dot(k, q, 1, 1) * SCALE
        if i == j:
            shape = (block, block)
            keep = lax.broadcasted_iota(jnp.int32, shape, 0) <= lax.broadcasted_iota(jnp.int32, shape, 1)
            s = jnp.where(keep, s, -jnp.inf)
        parts.append(s)
    top = functools.reduce(jnp.maximum, [jnp.max(s, 0, keepdims=True) for s in parts])
    parts = [jnp.exp(s - top) for s in parts]
    r = 1.0 / sum(jnp.sum(e, 0, keepdims=True) for e in parts)
    return q, [e * r for e in parts]


def local_forward_body(heads, block, q_ref, k_ref, v_ref, o_ref):
    for h in range(heads):
        vt = v_ref[:, cols(h)].T
        for j in range(q_ref.shape[0] // block):
            _, parts = probs_parts(q_ref, k_ref, h, j, block)
            acc = sum(
                dot(vt[:, i * block : (i + 1) * block], p.astype(bf16), 1, 0) for i, p in enumerate(parts)
            )
            o_ref[j * block : (j + 1) * block, cols(h)] = acc.T


def grad_mixed_body(*refs):
    pieces, w_ref, o_ref = refs[:-2], refs[-2], refs[-1]
    x = jnp.concatenate([p[...] for p in pieces], 0)
    o_ref[...] = dot(x, w_ref[...], 1, 1).astype(bf16)


def gather_grad(count, order, grads, g_ref):
    place = lax.axis_index("tp")
    for grad, masks in zip(grads, order):
        rows = grad.shape[0] // len(masks)
        for i, m in enumerate(masks):
            spot = pl.multiple_of(flipped(place, m, count) * rows, rows)
            g_ref[pl.ds(spot, rows), :] = grad[i * rows : (i + 1) * rows, :]


def segment_memory_grad(h, q_ref, qt_ref, g_ref, gate_ref, matrix, msum):
    qf = feat(q_ref[:, cols(h)].astype(f32))
    mem_out, r = read_memory(qf, matrix, msum)
    gmem = gate_ref[h : h + 1, :] * g_ref[:, cols(h)].astype(f32)
    gden = -jnp.sum(gmem * mem_out, 1, keepdims=True) * r
    both = halves(dot(qt_ref[2 * h * HD : 2 * (h + 1) * HD, :], side(*split(gmem * r)), 1, 0))
    return (both[:HD] + both[HD:]).astype(bf16), jnp.sum(gden * qf, 0, keepdims=True)


def memory_grad_first_body(group, count, order, steps, *refs):
    grads, (q_ref, qt_ref, gate_ref) = refs[: len(order)], refs[len(order) : len(order) + 3]
    recvs = refs[len(order) + 3 : len(order) + 3 + steps] + (None,)
    o_ref, g_ref = refs[-2:]
    gather_grad(count, order, grads, g_ref)
    sums = scan_state(False, recvs, slice(0, PAD))
    rows = []
    for h in group:
        matrix = scan_state(False, recvs, rows_of(h))
        o_ref[rows_of(h), :], row = segment_memory_grad(h, q_ref, qt_ref, g_ref, gate_ref, matrix, sums[h : h + 1, :])
        rows.append(row)
    o_ref[:PAD, :] = jnp.concatenate(rows + [jnp.zeros((PAD - len(rows), HD), f32)], 0).astype(bf16)


def memory_grad_second_body(first, group, first_ref, q_ref, qt_ref, gate_ref, g_ref, mem_ref, o_ref):
    cut = first_ref.shape[0]
    o_ref[:cut, :] = first_ref[...]
    rows = []
    for h in group:
        o_ref[rows_of(h), :], row = segment_memory_grad(h, q_ref, qt_ref, g_ref, gate_ref, *memory_of(mem_ref, h))
        rows.append(row)
    head = first_ref[:PAD, :].astype(f32)
    tail = [jnp.zeros((PAD - first - len(rows), HD), f32)]
    o_ref[:PAD, :] = jnp.concatenate([head[:first]] + rows + tail, 0).astype(bf16)


def flipped(place, mask, count):
    out = 0
    bit = 1
    while bit < count:
        own = (place // bit) % 2
        out = out + bit * ((1 - own) if mask & bit else own)
        bit *= 2
    return out


def mixed_rows(heads, count, masks, q_ref, mem_ref, lo_ref, gate_ref, mix_ref):
    place = lax.axis_index("tp")
    rows = q_ref.shape[0] // count
    for i, m in enumerate(masks):
        spot = pl.multiple_of(flipped(place, m, count) * rows, rows)
        for h in range(heads):
            qf = feat(q_ref[pl.ds(spot, rows), cols(h)].astype(f32))
            mem_out = read_memory(qf, *memory_of(mem_ref, h))[0]
            g = gate_ref[h : h + 1, :]
            x = g * mem_out + (1.0 - g) * lo_ref[pl.ds(spot, rows), cols(h)]
            mix_ref[i * rows : (i + 1) * rows, cols(h)] = x.astype(bf16)


def output_send_body(heads, count, masks, steps, q_ref, lo_ref, gate_ref, w_ref, *refs):
    recvs, (mem_ref, send_ref, mix_ref) = refs[:steps], refs[steps:]
    cut = recvs[-2].shape[0]
    for rows in (slice(0, cut), slice(cut, mem_ref.shape[0])):
        mem_ref[rows, :] = scan_state(False, recvs, rows)
    mixed_rows(heads, count, masks, q_ref, mem_ref, lo_ref, gate_ref, mix_ref)
    send_ref[...] = dot(mix_ref[...], w_ref[...], 1, 0).astype(bf16)


def output_keep_body(heads, count, masks, q_ref, mem_ref, lo_ref, gate_ref, w_ref, recv_ref, send_ref, keep_ref, mix_ref):
    mixed_rows(heads, count, masks, q_ref, mem_ref, lo_ref, gate_ref, mix_ref)
    total = dot(mix_ref[...], w_ref[...], 1, 0) + recv_ref[...].astype(f32)
    half = send_ref.shape[0]
    send_ref[...] = total[:half].astype(bf16)
    keep_ref[...] = total[half:]


def output_done_body(moves, keep_ref, recv_ref, *refs):
    gqs, (out_hbm, gq_hbm, out_ref, sems) = refs[: len(moves)], refs[len(moves) :]
    copies = [
        pltpu.make_async_copy(ref, gq_hbm.at[:, spots], sems.at[n]) for n, (ref, spots) in enumerate(zip(gqs, moves))
    ]
    out_ref[...] = (keep_ref[...] + recv_ref[...].astype(f32)).astype(bf16)
    copies = [pltpu.make_async_copy(out_ref, out_hbm, sems.at[len(moves)])] + copies
    for copy in copies:
        copy.start()
    for copy in copies:
        copy.wait()


def local_backward_body(group, block, q_ref, k_ref, v_ref, g_ref, mem_ref, gate_ref, *refs):
    gq_ref, gk_ref, gv_ref = refs
    blocks = q_ref.shape[0] // block
    for n, h in enumerate(group):
        g = gate_ref[h : h + 1, :]
        kt = k_ref[:, cols(h)].T
        gk = [None] * blocks
        gv = [None] * blocks

        def add(acc, i, x):
            acc[i] = x if acc[i] is None else acc[i] + x

        gq = []
        for j in range(blocks):
            q, parts = probs_parts(q_ref, k_ref, h, j, block)
            gl = ((1.0 - g) * g_ref[j * block : (j + 1) * block, cols(h)].astype(f32)).astype(bf16)
            gps = [dot(v_ref[i * block : (i + 1) * block, cols(h)], gl, 1, 1) for i in range(j + 1)]
            delta = sum(jnp.sum(p * gp, 0, keepdims=True) for p, gp in zip(parts, gps))
            acc = None
            for i, (p, gp) in enumerate(zip(parts, gps)):
                gs = (p * (gp - delta) * SCALE).astype(bf16)
                add(gk, i, dot(gs, q, 1, 0))
                add(gv, i, dot(p.astype(bf16), gl, 1, 0))
                t = dot(kt[:, i * block : (i + 1) * block], gs, 1, 0)
                acc = t if acc is None else acc + t
            gq.append(acc.T)
        for i in range(blocks):
            gk_ref[i * block : (i + 1) * block, cols(n)] = gk[i]
            gv_ref[i * block : (i + 1) * block, cols(n)] = gv[i]
        qx = q_ref[:, cols(h)].astype(f32)
        qf = feat(qx)
        matrix, msum = memory_of(mem_ref, h)
        mem_out, r = read_memory(qf, matrix, msum)
        gmem = g * g_ref[:, cols(h)].astype(f32)
        gden = -jnp.sum(gmem * mem_out, 1, keepdims=True) * r
        gqf = twofold(gmem * r, matrix, True) + gden * msum
        gq_ref[:, cols(n)] = (jnp.concatenate(gq, 0) + gqf * slope(qx)).astype(bf16)


def final_part(group, k_ref, v_ref, kl_ref, vl_ref, recvs, store):
    for i, h in enumerate(group):
        kx = k_ref[:, cols(h)].astype(f32)
        matrix = scan_state(True, recvs, rows_of(h))
        msum = scan_state(True, recvs, slice(0, PAD))[h : h + 1, :]
        gkf = halves(dot(v_ref[:, cols(h)], jnp.concatenate(split(matrix), 0), 1, 1)) + msum
        store(0, i, (kl_ref[:, cols(i)] + gkf * slope(kx)).astype(bf16))
        store(1, i, (vl_ref[:, cols(i)] + twofold(feat(kx), matrix)).astype(bf16))


def final_first_body(group, steps, *refs):
    outs = refs[-2:]

    def store(n, i, x):
        outs[n][:, cols(i)] = x

    final_part(group, *refs[:4], refs[4 : 4 + steps] + (None,), store)


def final_second_body(before, group, steps, *refs):
    firsts = refs[4 + steps : 6 + steps]
    outs, parts, sems = refs[-5:-3], refs[-3:-1], refs[-1]
    copies = []

    def send(ref, out, spots, sem):
        copies.append(pltpu.make_async_copy(ref, out.at[:, spots], sem))
        copies[-1].start()

    for n in range(2):
        send(firsts[n], outs[n], slice(0, before * HD), sems.at[n, len(group)])

    def store(n, i, x):
        parts[n][:, cols(i)] = x
        send(parts[n].at[:, cols(i)], outs[n], cols(group[i]), sems.at[n, i])

    final_part(group, *refs[:4], refs[4 : 4 + steps], store)
    for copy in copies:
        copy.wait()


def swap(x, axis, bit):
    count = lax.axis_size(axis)
    return lax.ppermute(x, axis, [(i, i ^ bit) for i in range(count)])


def scan(own, axis, cut):
    count = lax.axis_size(axis)
    recvs = []
    bit = 1
    while bit < count:
        have = [own] + recvs
        shapes = [own.shape]
        ends = bit * 2 == count
        if ends:
            shapes = [(cut, HD), (own.shape[0] - cut, HD)]
        sends = [own]
        if len(have) > 1 or ends:
            body = functools.partial(add_body, len(have))
            outs = [(shape, bf16) for shape in shapes]
            sends = call(body, outs, [VM] * len(have), flops=1 << 20)(*have)
        for send in sends:
            recvs.append(swap(send, axis, bit))
        bit *= 2
    return recvs


def reverse_bits(value, count):
    out = 0
    bit = 1
    while bit < count:
        out = out * 2 + (1 if value & bit else 0)
        bit *= 2
    return out


def local(query, keys, values, beta, out_weight, cotangent):
    length, width = query.shape
    heads = width // HD
    model = out_weight.shape[1]
    tp = lax.axis_size("tp")
    block = min(256, length)
    packed = (heads * HD + PAD, HD)
    hbm = pl.BlockSpec(memory_space=pltpu.HBM)
    full = (length, width)
    first = -(-heads // 2)
    groups = [list(range(first)), list(range(first, heads))]
    cut = PAD + first * HD

    def in_hbm(*xs):
        return [pltpu.with_memory_space_constraint(x, pltpu.HBM) for x in xs]

    own, keys, values = call(
        functools.partial(own_memory_body, heads),
        [(packed, bf16), (full, bf16), (full, bf16)],
        [hbm] * 2,
        scratch=[pltpu.SemaphoreType.DMA((2, heads))],
    )(*in_hbm(keys, values))
    query, query_t, gates = call(
        functools.partial(load_query_body, heads),
        [(full, bf16), ((2 * width, length), bf16), ((-(-heads // 8) * 8, HD), f32)],
        [hbm] * 2,
        scratch=[pltpu.SMEM((heads,), f32), pltpu.SemaphoreType.DMA((heads + 1,))],
        flops=1 << 16,
    )(*in_hbm(query, beta))
    fwd = scan(own, "seq", cut)

    held = {0: cotangent}
    order, later = [[0]], []
    if tp > 1:
        held[1] = swap(cotangent, "tp", 1)
        order = [[0, 1]]
    bit = 2
    far = [0]
    while bit < tp:
        for m in list(far):
            held[m | bit] = swap(held[m], "tp", bit)
            far.append(m | bit)
        bit *= 2
    for m in far[1:]:
        held[m | 1] = swap(held[m], "tp", 1)
        later += [m, m | 1]
    order += [later] if later else []

    local_out = call(
        functools.partial(local_forward_body, heads, block), [(full, f32)], [VM, VM, VM]
    )(query, keys, values)[0]

    grads = []
    for masks in order:
        rows = cotangent.shape[0] * len(masks)
        grads.append(
            call(
                grad_mixed_body, [((rows, width), bf16)], [VM] * (len(masks) + 1)
            )(*[held[m] for m in masks], out_weight)[0]
        )

    places = [reverse_bits(tp - 1 - i, tp) for i in range(tp)]
    half = tp // 2
    steps = len(fwd)
    part, grad = call(
        functools.partial(memory_grad_first_body, groups[0], tp, order, steps - 1),
        [((cut, HD), bf16), (full, bf16)],
        [VM] * (len(order) + 2 + steps),
    )(*grads, query, query_t, gates, *fwd[:-1])
    memory, send = call(
        functools.partial(output_send_body, heads, tp, places[:half], steps),
        [(packed, f32), ((length // 2, model), bf16)],
        [VM] * (4 + steps),
        scratch=[pltpu.VMEM((length // 2, width), bf16)],
    )(query, local_out, gates, out_weight, *fwd)
    recv = swap(send, "tp", 1)
    memory_grad = call(
        functools.partial(memory_grad_second_body, first, groups[1]), [(packed, bf16)], [VM] * 6
    )(part, query, query_t, gates, grad, memory)[0]
    bwd = scan(memory_grad, "seq", cut)

    quarter = length // 4
    send, keep = call(
        functools.partial(output_keep_body, heads, tp, places[half:]),
        [((quarter, model), bf16), ((quarter, model), f32)],
        [VM] * 6,
        scratch=[pltpu.VMEM((length // 2, width), bf16)],
    )(query, memory, local_out, gates, out_weight, recv)
    bit = 2
    while 2 * bit < tp:
        total = keep + swap(send, "tp", bit).astype(f32)
        part = total.shape[0] // 2
        send, keep = total[:part].astype(bf16), total[part:]
        bit *= 2
    recv = swap(send, "tp", bit)
    pieces = []
    for group in groups:
        part = (length, len(group) * HD)
        pieces.append(
            call(
                functools.partial(local_backward_body, group, block),
                [(part, bf16), (part, f32), (part, f32)],
                [VM] * 6,
            )(query, keys, values, grad, memory, gates)
        )
    own_rows = (length // tp, model)
    output, grad_query = call(
        functools.partial(output_done_body, [slice(g[0] * HD, (g[-1] + 1) * HD) for g in groups]),
        [(own_rows, bf16), (full, bf16)],
        [VM] * (2 + len(groups)),
        out_specs=[hbm] * 2,
        scratch=[pltpu.VMEM(own_rows, bf16), pltpu.SemaphoreType.DMA((len(groups) + 1,))],
        flops=1 << 20,
    )(keep, recv, *[piece[0] for piece in pieces])
    part = (length, first * HD)
    early = call(
        functools.partial(final_first_body, groups[0], len(bwd) - 1),
        [(part, bf16)] * 2,
        [VM] * (3 + len(bwd)),
    )(keys, values, *pieces[0][1:], *bwd[:-1])
    part = (length, len(groups[1]) * HD)
    grad_keys, grad_values = call(
        functools.partial(final_second_body, first, groups[1], len(bwd)),
        [(full, bf16)] * 2,
        [VM] * (6 + len(bwd)),
        out_specs=[hbm] * 2,
        scratch=[
            pltpu.VMEM(part, bf16),
            pltpu.VMEM(part, bf16),
            pltpu.SemaphoreType.DMA((2, len(groups[1]) + 1)),
        ],
    )(keys, values, *pieces[1][1:], *bwd, *early)
    return (output, grad_query, grad_keys, grad_values)


def solution(mesh):
    in_specs = (
        P("seq", "tp"),
        P("seq", "tp"),
        P("seq", "tp"),
        P("tp"),
        P("tp", None),
        P(("seq", "tp"), None),
    )
    out_specs = (P(("seq", "tp"), None), P("seq", "tp"), P("seq", "tp"), P("seq", "tp"))

    return jax.shard_map(local, mesh=mesh, in_specs=in_specs, out_specs=out_specs, check_vma=False)
```

```python
import functools

import jax
import jax.numpy as jnp
from jax import lax
from jax.experimental import pallas as pl
from jax.experimental.pallas import tpu as pltpu
from jax.sharding import PartitionSpec as P


HD = 128
PAD = 16
SCALE = HD ** (-0.5)

f32 = jnp.float32
bf16 = jnp.bfloat16

VM = pl.BlockSpec(memory_space=pltpu.VMEM)


def dot(a, b, ca, cb):
    return lax.dot_general(a, b, (((ca,), (cb,)), ((), ())), preferred_element_type=f32)


def split(x):
    hi = x.astype(bf16)
    return hi, (x - hi.astype(f32)).astype(bf16)


def side(a, b):
    return jnp.concatenate([a, b], 1)


def halves(y):
    return y[:, : y.shape[1] // 2] + y[:, y.shape[1] // 2 :]


def twofold(x, m, transposed=False):
    mh, ml = split(m)
    both = jnp.concatenate([mh, ml], 0) if transposed else side(mh, ml)
    if transposed:
        return halves(dot(side(*split(x)), side(both, both), 1, 1))
    return halves(dot(side(*split(x)), jnp.concatenate([both, both], 0), 1, 0))


def feat(x):
    return jnp.where(x > 0, x + 1.0, jnp.exp(jnp.minimum(x, 0.0)))


def slope(x):
    return jnp.where(x > 0, 1.0, jnp.exp(jnp.minimum(x, 0.0)))


def cols(h):
    return slice(h * HD, (h + 1) * HD)


def pair(h):
    return slice(2 * h * HD, 2 * (h + 1) * HD)


def call(body, outs, specs, out_specs=None, scratch=(), flops=1 << 28, vmem=24, alias=None):
    if out_specs is None:
        out_specs = [VM] * len(outs)
    return pl.pallas_call(
        body,
        out_shape=[jax.ShapeDtypeStruct(s, d) for s, d in outs],
        in_specs=specs,
        out_specs=out_specs,
        scratch_shapes=list(scratch),
        input_output_aliases=alias or {},
        compiler_params=pltpu.CompilerParams(vmem_limit_bytes=vmem << 20),
        cost_estimate=pl.CostEstimate(flops=flops, transcendentals=0, bytes_accessed=1 << 20),
    )


def pad_rows(rows):
    return jnp.concatenate(rows + [jnp.zeros((PAD - len(rows), HD), f32)], 0).astype(bf16)


def rows_of(h):
    return slice(PAD + h * HD, PAD + (h + 1) * HD)


def memory_of(mem_ref, h):
    return mem_ref[rows_of(h), :], mem_ref[h : h + 1, :]


def own_memory_body(heads, k_hbm, v_hbm, o_ref, k_ref, v_ref, sems):
    part = k_ref.shape[0] // heads
    blocks = [slice(i * part, (i + 1) * part) for i in range(heads)]
    copies = [
        [pltpu.make_async_copy(a.at[rows], b.at[rows], sems.at[i, n]) for i, (a, b) in enumerate(((k_hbm, k_ref), (v_hbm, v_ref)))]
        for n, rows in enumerate(blocks)
    ]
    for pair in copies:
        for copy in pair:
            copy.start()
    both = [None] * heads
    sums = [None] * heads
    for rows, pair in zip(blocks, copies):
        for copy in pair:
            copy.wait()
        for h in range(heads):
            kf = feat(k_ref[rows, cols(h)].astype(f32))
            x = dot(side(*split(kf)), v_ref[rows, cols(h)], 0, 0)
            y = jnp.sum(kf, 0, keepdims=True)
            both[h] = x if both[h] is None else both[h] + x
            sums[h] = y if sums[h] is None else sums[h] + y
    for h in range(heads):
        o_ref[rows_of(h), :] = (both[h][:HD] + both[h][HD:]).astype(bf16)
    o_ref[:PAD, :] = pad_rows(sums)


def load_query_body(heads, q_hbm, beta_hbm, q_ref, qf_ref, qs_ref, qt_ref, gate_ref, beta_ref, sems):
    rows = q_ref.shape[0] // heads
    beta_copy = pltpu.make_async_copy(beta_hbm, beta_ref, sems.at[heads])
    beta_copy.start()
    parts = [pl.ds(i * rows, rows) for i in range(heads)]
    copies = [pltpu.make_async_copy(q_hbm.at[p], q_ref.at[p], sems.at[i]) for i, p in enumerate(parts)]
    for copy in copies:
        copy.start()
    beta_copy.wait()
    for h in range(heads):
        gate_ref[h : h + 1, :] = jax.nn.sigmoid(jnp.full((1, HD), beta_ref[h], f32))
    for copy in copies:
        copy.wait()
    for h in range(heads):
        qf = feat(q_ref[:, cols(h)].astype(f32))
        both = side(*split(qf))
        qf_ref[:, cols(h)] = qf
        qs_ref[:, pair(h)] = both
        qt_ref[pair(h), :] = both.T


def add_body(count, *refs):
    total = refs[0][...].astype(f32)
    for ref in refs[1:count]:
        total = total + ref[...].astype(f32)
    start = 0
    for out in refs[count:]:
        out[...] = total[start : start + out.shape[0]].astype(bf16)
        start += out.shape[0]


def scan_state(backward, refs, rows):
    place = lax.axis_index("seq")
    cut = refs[-2].shape[0] if refs[-1] is not None else None
    state = None
    for i, ref in enumerate(refs[:-1]):
        upper = (place // (1 << i)) % 2
        take = (1 - upper if backward else upper).astype(f32)
        part = rows
        if i == len(refs) - 2 and cut is not None and rows.start >= cut:
            ref, part = refs[-1], slice(rows.start - cut, rows.stop - cut)
        x = ref[part, :].astype(f32) * take
        state = x if state is None else state + x
    return state


def read_memory(qf, qs, matrix, msum):
    both = side(*split(matrix))
    numer = halves(dot(qs, jnp.concatenate([both, both], 0), 1, 0))
    r = 1.0 / (jnp.sum(qf * msum, 1, keepdims=True) + 1.0)
    return numer * r, r


def probs_parts(q_ref, k_ref, h, j, block):
    q = q_ref[j * block : (j + 1) * block, cols(h)]
    parts = []
    for i in range(j + 1):
        k = k_ref[i * block : (i + 1) * block, cols(h)]
        s = dot(k, q, 1, 1) * SCALE
        if i == j:
            shape = (block, block)
            keep = lax.broadcasted_iota(jnp.int32, shape, 0) <= lax.broadcasted_iota(jnp.int32, shape, 1)
            s = jnp.where(keep, s, -jnp.inf)
        parts.append(s)
    top = functools.reduce(jnp.maximum, [jnp.max(s, 0, keepdims=True) for s in parts])
    parts = [jnp.exp(s - top) for s in parts]
    r = 1.0 / sum(jnp.sum(e, 0, keepdims=True) for e in parts)
    return q, [e * r for e in parts]


def local_forward_body(heads, block, q_ref, k_ref, v_ref, o_ref):
    for h in range(heads):
        vt = v_ref[:, cols(h)].T
        for j in range(q_ref.shape[0] // block):
            _, parts = probs_parts(q_ref, k_ref, h, j, block)
            acc = sum(
                dot(vt[:, i * block : (i + 1) * block], p.astype(bf16), 1, 0) for i, p in enumerate(parts)
            )
            o_ref[j * block : (j + 1) * block, cols(h)] = acc.T


def grad_mixed_body(*refs):
    pieces, w_ref, o_ref = refs[:-2], refs[-2], refs[-1]
    x = jnp.concatenate([p[...] for p in pieces], 0)
    o_ref[...] = dot(x, w_ref[...], 1, 1).astype(bf16)


def gather_grad(count, order, grads, g_ref):
    place = lax.axis_index("tp")
    for grad, masks in zip(grads, order):
        rows = grad.shape[0] // len(masks)
        for i, m in enumerate(masks):
            spot = pl.multiple_of(flipped(place, m, count) * rows, rows)
            g_ref[pl.ds(spot, rows), :] = grad[i * rows : (i + 1) * rows, :]


def segment_memory_grad(h, qf_ref, qs_ref, qt_ref, g_ref, gate_ref, matrix, msum):
    qf = qf_ref[:, cols(h)]
    mem_out, r = read_memory(qf, qs_ref[:, pair(h)], matrix, msum)
    gmem = gate_ref[h : h + 1, :] * g_ref[:, cols(h)].astype(f32)
    gden = -jnp.sum(gmem * mem_out, 1, keepdims=True) * r
    both = halves(dot(qt_ref[pair(h), :], side(*split(gmem * r)), 1, 0))
    return (both[:HD] + both[HD:]).astype(bf16), jnp.sum(gden * qf, 0, keepdims=True)


def memory_grad_first_body(group, count, order, steps, *refs):
    grads, (qf_ref, qs_ref, qt_ref, gate_ref) = refs[: len(order)], refs[len(order) : len(order) + 4]
    recvs = refs[len(order) + 4 : len(order) + 4 + steps] + (None,)
    o_ref, g_ref = refs[-2:]
    gather_grad(count, order, grads, g_ref)
    sums = scan_state(False, recvs, slice(0, PAD))
    rows = []
    for h in group:
        matrix = scan_state(False, recvs, rows_of(h))
        o_ref[rows_of(h), :], row = segment_memory_grad(
            h, qf_ref, qs_ref, qt_ref, g_ref, gate_ref, matrix, sums[h : h + 1, :]
        )
        rows.append(row)
    o_ref[:PAD, :] = jnp.concatenate(rows + [jnp.zeros((PAD - len(rows), HD), f32)], 0).astype(bf16)


def memory_grad_second_body(first, group, first_ref, qf_ref, qs_ref, qt_ref, gate_ref, g_ref, mem_ref, o_ref):
    cut = first_ref.shape[0]
    o_ref[:cut, :] = first_ref[...]
    rows = []
    for h in group:
        o_ref[rows_of(h), :], row = segment_memory_grad(
            h, qf_ref, qs_ref, qt_ref, g_ref, gate_ref, *memory_of(mem_ref, h)
        )
        rows.append(row)
    head = first_ref[:PAD, :].astype(f32)
    tail = [jnp.zeros((PAD - first - len(rows), HD), f32)]
    o_ref[:PAD, :] = jnp.concatenate([head[:first]] + rows + tail, 0).astype(bf16)


def flipped(place, mask, count):
    out = 0
    bit = 1
    while bit < count:
        own = (place // bit) % 2
        out = out + bit * ((1 - own) if mask & bit else own)
        bit *= 2
    return out


def mixed_rows(heads, count, masks, qf_ref, qs_ref, mem_ref, lo_ref, gate_ref, mix_ref):
    place = lax.axis_index("tp")
    rows = qf_ref.shape[0] // count
    for i, m in enumerate(masks):
        spot = pl.multiple_of(flipped(place, m, count) * rows, rows)
        for h in range(heads):
            qf, qs = qf_ref[pl.ds(spot, rows), cols(h)], qs_ref[pl.ds(spot, rows), pair(h)]
            mem_out = read_memory(qf, qs, *memory_of(mem_ref, h))[0]
            g = gate_ref[h : h + 1, :]
            x = g * mem_out + (1.0 - g) * lo_ref[pl.ds(spot, rows), cols(h)]
            mix_ref[i * rows : (i + 1) * rows, cols(h)] = x.astype(bf16)


def output_send_body(heads, count, masks, steps, qf_ref, qs_ref, lo_ref, gate_ref, w_ref, *refs):
    recvs, (mem_ref, send_ref, mix_ref) = refs[:steps], refs[steps:]
    cut = recvs[-2].shape[0]
    for rows in (slice(0, cut), slice(cut, mem_ref.shape[0])):
        mem_ref[rows, :] = scan_state(False, recvs, rows)
    mixed_rows(heads, count, masks, qf_ref, qs_ref, mem_ref, lo_ref, gate_ref, mix_ref)
    send_ref[...] = dot(mix_ref[...], w_ref[...], 1, 0).astype(bf16)


def output_keep_body(
    heads, count, masks, qf_ref, qs_ref, mem_ref, lo_ref, gate_ref, w_ref, recv_ref, send_ref, keep_ref, mix_ref
):
    mixed_rows(heads, count, masks, qf_ref, qs_ref, mem_ref, lo_ref, gate_ref, mix_ref)
    total = dot(mix_ref[...], w_ref[...], 1, 0) + recv_ref[...].astype(f32)
    half = send_ref.shape[0]
    send_ref[...] = total[:half].astype(bf16)
    keep_ref[...] = total[half:]


def output_done_body(moves, keep_ref, recv_ref, *refs):
    gqs, (out_hbm, gq_hbm, out_ref, sems) = refs[: len(moves)], refs[len(moves) :]
    copies = [
        pltpu.make_async_copy(ref, gq_hbm.at[:, spots], sems.at[n]) for n, (ref, spots) in enumerate(zip(gqs, moves))
    ]
    out_ref[...] = (keep_ref[...] + recv_ref[...].astype(f32)).astype(bf16)
    copies = [pltpu.make_async_copy(out_ref, out_hbm, sems.at[len(moves)])] + copies
    for copy in copies:
        copy.start()
    for copy in copies:
        copy.wait()


def local_backward_body(
    group, block, q_ref, qf_ref, qs_ref, k_ref, v_ref, g_ref, mem_ref, gate_ref, *refs
):
    gq_ref, gk_ref, gv_ref = refs
    blocks = q_ref.shape[0] // block
    for n, h in enumerate(group):
        g = gate_ref[h : h + 1, :]
        kt = k_ref[:, cols(h)].T
        gk = [None] * blocks
        gv = [None] * blocks

        def add(acc, i, x):
            acc[i] = x if acc[i] is None else acc[i] + x

        gq = []
        for j in range(blocks):
            q, parts = probs_parts(q_ref, k_ref, h, j, block)
            gl = ((1.0 - g) * g_ref[j * block : (j + 1) * block, cols(h)].astype(f32)).astype(bf16)
            gps = [dot(v_ref[i * block : (i + 1) * block, cols(h)], gl, 1, 1) for i in range(j + 1)]
            delta = sum(jnp.sum(p * gp, 0, keepdims=True) for p, gp in zip(parts, gps))
            acc = None
            for i, (p, gp) in enumerate(zip(parts, gps)):
                gs = (p * (gp - delta) * SCALE).astype(bf16)
                add(gk, i, dot(gs, q, 1, 0))
                add(gv, i, dot(p.astype(bf16), gl, 1, 0))
                t = dot(kt[:, i * block : (i + 1) * block], gs, 1, 0)
                acc = t if acc is None else acc + t
            gq.append(acc.T)
        for i in range(blocks):
            gk_ref[i * block : (i + 1) * block, cols(n)] = gk[i]
            gv_ref[i * block : (i + 1) * block, cols(n)] = gv[i]
        qx = q_ref[:, cols(h)].astype(f32)
        matrix, msum = memory_of(mem_ref, h)
        mem_out, r = read_memory(qf_ref[:, cols(h)], qs_ref[:, pair(h)], matrix, msum)
        gmem = g * g_ref[:, cols(h)].astype(f32)
        gden = -jnp.sum(gmem * mem_out, 1, keepdims=True) * r
        gqf = twofold(gmem * r, matrix, True) + gden * msum
        gq_ref[:, cols(n)] = (jnp.concatenate(gq, 0) + gqf * slope(qx)).astype(bf16)


def final_part(group, k_ref, v_ref, kl_ref, vl_ref, recvs, store):
    for i, h in enumerate(group):
        kx = k_ref[:, cols(h)].astype(f32)
        matrix = scan_state(True, recvs, rows_of(h))
        msum = scan_state(True, recvs, slice(0, PAD))[h : h + 1, :]
        gkf = halves(dot(v_ref[:, cols(h)], jnp.concatenate(split(matrix), 0), 1, 1)) + msum
        store(0, i, (kl_ref[:, cols(i)] + gkf * slope(kx)).astype(bf16))
        store(1, i, (vl_ref[:, cols(i)] + twofold(feat(kx), matrix)).astype(bf16))


def final_first_body(group, steps, *refs):
    outs = refs[-2:]

    def store(n, i, x):
        outs[n][:, cols(i)] = x

    final_part(group, *refs[:4], refs[4 : 4 + steps] + (None,), store)


def final_second_body(before, group, steps, *refs):
    firsts = refs[4 + steps : 6 + steps]
    outs, parts, sems = refs[-5:-3], refs[-3:-1], refs[-1]
    copies = []

    def send(ref, out, spots, sem):
        copies.append(pltpu.make_async_copy(ref, out.at[:, spots], sem))
        copies[-1].start()

    for n in range(2):
        send(firsts[n], outs[n], slice(0, before * HD), sems.at[n, len(group)])

    def store(n, i, x):
        parts[n][:, cols(i)] = x
        send(parts[n].at[:, cols(i)], outs[n], cols(group[i]), sems.at[n, i])

    final_part(group, *refs[:4], refs[4 : 4 + steps], store)
    for copy in copies:
        copy.wait()


def swap(x, axis, bit):
    count = lax.axis_size(axis)
    return lax.ppermute(x, axis, [(i, i ^ bit) for i in range(count)])


def scan(own, axis, cut):
    count = lax.axis_size(axis)
    recvs = []
    bit = 1
    while bit < count:
        have = [own] + recvs
        shapes = [own.shape]
        ends = bit * 2 == count
        if ends:
            shapes = [(cut, HD), (own.shape[0] - cut, HD)]
        sends = [own]
        if len(have) > 1 or ends:
            body = functools.partial(add_body, len(have))
            outs = [(shape, bf16) for shape in shapes]
            sends = call(body, outs, [VM] * len(have), flops=1 << 20)(*have)
        for send in sends:
            recvs.append(swap(send, axis, bit))
        bit *= 2
    return recvs


def reverse_bits(value, count):
    out = 0
    bit = 1
    while bit < count:
        out = out * 2 + (1 if value & bit else 0)
        bit *= 2
    return out


def local(query, keys, values, beta, out_weight, cotangent):
    length, width = query.shape
    heads = width // HD
    model = out_weight.shape[1]
    tp = lax.axis_size("tp")
    block = min(256, length)
    packed = (heads * HD + PAD, HD)
    hbm = pl.BlockSpec(memory_space=pltpu.HBM)
    full = (length, width)
    first = -(-heads // 2)
    groups = [list(range(first)), list(range(first, heads))]
    cut = PAD + first * HD

    def in_hbm(*xs):
        return [pltpu.with_memory_space_constraint(x, pltpu.HBM) for x in xs]

    own, keys, values = call(
        functools.partial(own_memory_body, heads),
        [(packed, bf16), (full, bf16), (full, bf16)],
        [hbm] * 2,
        scratch=[pltpu.SemaphoreType.DMA((2, heads))],
    )(*in_hbm(keys, values))
    query, feats, feats_s, feats_t, gates = call(
        functools.partial(load_query_body, heads),
        [(full, bf16), (full, f32), ((length, 2 * width), bf16), ((2 * width, length), bf16), ((-(-heads // 8) * 8, HD), f32)],
        [hbm] * 2,
        scratch=[pltpu.SMEM((heads,), f32), pltpu.SemaphoreType.DMA((heads + 1,))],
        flops=1 << 16,
    )(*in_hbm(query, beta))
    fwd = scan(own, "seq", cut)

    held = {0: cotangent}
    order, later = [[0]], []
    if tp > 1:
        held[1] = swap(cotangent, "tp", 1)
        order = [[0, 1]]
    bit = 2
    far = [0]
    while bit < tp:
        for m in list(far):
            held[m | bit] = swap(held[m], "tp", bit)
            far.append(m | bit)
        bit *= 2
    for m in far[1:]:
        held[m | 1] = swap(held[m], "tp", 1)
        later += [m, m | 1]
    order += [later] if later else []

    local_out = call(
        functools.partial(local_forward_body, heads, block), [(full, f32)], [VM, VM, VM]
    )(query, keys, values)[0]

    grads = []
    for masks in order:
        rows = cotangent.shape[0] * len(masks)
        grads.append(
            call(
                grad_mixed_body, [((rows, width), bf16)], [VM] * (len(masks) + 1)
            )(*[held[m] for m in masks], out_weight)[0]
        )

    places = [reverse_bits(tp - 1 - i, tp) for i in range(tp)]
    half = tp // 2
    steps = len(fwd)
    part, grad = call(
        functools.partial(memory_grad_first_body, groups[0], tp, order, steps - 1),
        [((cut, HD), bf16), (full, bf16)],
        [VM] * (len(order) + 3 + steps),
    )(*grads, feats, feats_s, feats_t, gates, *fwd[:-1])
    memory, send = call(
        functools.partial(output_send_body, heads, tp, places[:half], steps),
        [(packed, f32), ((length // 2, model), bf16)],
        [VM] * (5 + steps),
        scratch=[pltpu.VMEM((length // 2, width), bf16)],
    )(feats, feats_s, local_out, gates, out_weight, *fwd)
    recv = swap(send, "tp", 1)
    memory_grad = call(
        functools.partial(memory_grad_second_body, first, groups[1]), [(packed, bf16)], [VM] * 7
    )(part, feats, feats_s, feats_t, gates, grad, memory)[0]
    bwd = scan(memory_grad, "seq", cut)

    quarter = length // 4
    send, keep = call(
        functools.partial(output_keep_body, heads, tp, places[half:]),
        [((quarter, model), bf16), ((quarter, model), f32)],
        [VM] * 7,
        scratch=[pltpu.VMEM((length // 2, width), bf16)],
    )(feats, feats_s, memory, local_out, gates, out_weight, recv)
    bit = 2
    while 2 * bit < tp:
        total = keep + swap(send, "tp", bit).astype(f32)
        part = total.shape[0] // 2
        send, keep = total[:part].astype(bf16), total[part:]
        bit *= 2
    recv = swap(send, "tp", bit)
    pieces = []
    for group in groups:
        part = (length, len(group) * HD)
        pieces.append(
            call(
                functools.partial(local_backward_body, group, block),
                [(part, bf16), (part, f32), (part, f32)],
                [VM] * 8,
            )(query, feats, feats_s, keys, values, grad, memory, gates)
        )
    own_rows = (length // tp, model)
    output, grad_query = call(
        functools.partial(output_done_body, [slice(g[0] * HD, (g[-1] + 1) * HD) for g in groups]),
        [(own_rows, bf16), (full, bf16)],
        [VM] * (2 + len(groups)),
        out_specs=[hbm] * 2,
        scratch=[pltpu.VMEM(own_rows, bf16), pltpu.SemaphoreType.DMA((len(groups) + 1,))],
        flops=1 << 20,
    )(keep, recv, *[piece[0] for piece in pieces])
    part = (length, first * HD)
    early = call(
        functools.partial(final_first_body, groups[0], len(bwd) - 1),
        [(part, bf16)] * 2,
        [VM] * (3 + len(bwd)),
    )(keys, values, *pieces[0][1:], *bwd[:-1])
    part = (length, len(groups[1]) * HD)
    grad_keys, grad_values = call(
        functools.partial(final_second_body, first, groups[1], len(bwd)),
        [(full, bf16)] * 2,
        [VM] * (6 + len(bwd)),
        out_specs=[hbm] * 2,
        scratch=[
            pltpu.VMEM(part, bf16),
            pltpu.VMEM(part, bf16),
            pltpu.SemaphoreType.DMA((2, len(groups[1]) + 1)),
        ],
    )(keys, values, *pieces[1][1:], *bwd, *early)
    return (output, grad_query, grad_keys, grad_values)


def solution(mesh):
    in_specs = (
        P("seq", "tp"),
        P("seq", "tp"),
        P("seq", "tp"),
        P("tp"),
        P("tp", None),
        P(("seq", "tp"), None),
    )
    out_specs = (P(("seq", "tp"), None), P("seq", "tp"), P("seq", "tp"), P("seq", "tp"))

    return jax.shard_map(local, mesh=mesh, in_specs=in_specs, out_specs=out_specs, check_vma=False)
```

```python
import functools

import jax
import jax.numpy as jnp
from jax import lax
from jax.experimental import pallas as pl
from jax.experimental.pallas import tpu as pltpu
from jax.sharding import PartitionSpec as P


HD = 128
PAD = 16
SCALE = HD ** (-0.5)

f32 = jnp.float32
bf16 = jnp.bfloat16

VM = pl.BlockSpec(memory_space=pltpu.VMEM)


def dot(a, b, ca, cb):
    return lax.dot_general(a, b, (((ca,), (cb,)), ((), ())), preferred_element_type=f32)


def split(x):
    hi = x.astype(bf16)
    return hi, (x - hi.astype(f32)).astype(bf16)


def side(a, b):
    return jnp.concatenate([a, b], 1)


def halves(y):
    return y[:, : y.shape[1] // 2] + y[:, y.shape[1] // 2 :]


def twofold(x, m, transposed=False):
    mh, ml = split(m)
    both = jnp.concatenate([mh, ml], 0) if transposed else side(mh, ml)
    if transposed:
        return halves(dot(side(*split(x)), side(both, both), 1, 1))
    return halves(dot(side(*split(x)), jnp.concatenate([both, both], 0), 1, 0))


def feat(x):
    return jnp.where(x > 0, x + 1.0, jnp.exp(jnp.minimum(x, 0.0)))


def slope(x):
    return jnp.where(x > 0, 1.0, jnp.exp(jnp.minimum(x, 0.0)))


def cols(h):
    return slice(h * HD, (h + 1) * HD)


def pair(h):
    return slice(2 * h * HD, 2 * (h + 1) * HD)


def call(body, outs, specs, out_specs=None, scratch=(), flops=1 << 28, vmem=24, alias=None):
    if out_specs is None:
        out_specs = [VM] * len(outs)
    return pl.pallas_call(
        body,
        out_shape=[jax.ShapeDtypeStruct(s, d) for s, d in outs],
        in_specs=specs,
        out_specs=out_specs,
        scratch_shapes=list(scratch),
        input_output_aliases=alias or {},
        compiler_params=pltpu.CompilerParams(vmem_limit_bytes=vmem << 20),
        cost_estimate=pl.CostEstimate(flops=flops, transcendentals=0, bytes_accessed=1 << 20),
    )


def pad_rows(rows):
    return jnp.concatenate(rows + [jnp.zeros((PAD - len(rows), HD), f32)], 0).astype(bf16)


def rows_of(h):
    return slice(PAD + h * HD, PAD + (h + 1) * HD)


def memory_of(mem_ref, h):
    return mem_ref[rows_of(h), :], mem_ref[h : h + 1, :]


def own_memory_body(heads, k_hbm, v_hbm, o_ref, k_ref, v_ref, sems):
    part = k_ref.shape[0] // heads
    blocks = [slice(i * part, (i + 1) * part) for i in range(heads)]
    copies = [
        [pltpu.make_async_copy(a.at[rows], b.at[rows], sems.at[i, n]) for i, (a, b) in enumerate(((k_hbm, k_ref), (v_hbm, v_ref)))]
        for n, rows in enumerate(blocks)
    ]
    for pair in copies:
        for copy in pair:
            copy.start()
    both = [None] * heads
    sums = [None] * heads
    for rows, pair in zip(blocks, copies):
        for copy in pair:
            copy.wait()
        for h in range(heads):
            kf = feat(k_ref[rows, cols(h)].astype(f32))
            x = dot(side(*split(kf)), v_ref[rows, cols(h)], 0, 0)
            y = jnp.sum(kf, 0, keepdims=True)
            both[h] = x if both[h] is None else both[h] + x
            sums[h] = y if sums[h] is None else sums[h] + y
    for h in range(heads):
        o_ref[rows_of(h), :] = (both[h][:HD] + both[h][HD:]).astype(bf16)
    o_ref[:PAD, :] = pad_rows(sums)


def load_query_body(heads, q_hbm, beta_hbm, q_ref, qf_ref, qs_ref, qt_ref, gate_ref, beta_ref, sems):
    rows = q_ref.shape[0] // heads
    beta_copy = pltpu.make_async_copy(beta_hbm, beta_ref, sems.at[heads])
    beta_copy.start()
    parts = [pl.ds(i * rows, rows) for i in range(heads)]
    copies = [pltpu.make_async_copy(q_hbm.at[p], q_ref.at[p], sems.at[i]) for i, p in enumerate(parts)]
    for copy in copies:
        copy.start()
    beta_copy.wait()
    for h in range(heads):
        gate_ref[h : h + 1, :] = jax.nn.sigmoid(jnp.full((1, HD), beta_ref[h], f32))
    for copy in copies:
        copy.wait()
    for h in range(heads):
        qf = feat(q_ref[:, cols(h)].astype(f32))
        both = side(*split(qf))
        qf_ref[:, cols(h)] = qf
        qs_ref[:, pair(h)] = both
        qt_ref[pair(h), :] = both.T


def add_body(count, *refs):
    total = refs[0][...].astype(f32)
    for ref in refs[1:count]:
        total = total + ref[...].astype(f32)
    start = 0
    for out in refs[count:]:
        out[...] = total[start : start + out.shape[0]].astype(bf16)
        start += out.shape[0]


def scan_state(backward, refs, rows):
    place = lax.axis_index("seq")
    cut = refs[-2].shape[0] if refs[-1] is not None else None
    state = None
    for i, ref in enumerate(refs[:-1]):
        upper = (place // (1 << i)) % 2
        take = (1 - upper if backward else upper).astype(f32)
        part = rows
        if i == len(refs) - 2 and cut is not None and rows.start >= cut:
            ref, part = refs[-1], slice(rows.start - cut, rows.stop - cut)
        x = ref[part, :].astype(f32) * take
        state = x if state is None else state + x
    return state


def read_memory(qf, qs, matrix, msum):
    both = side(*split(matrix))
    numer = halves(dot(qs, jnp.concatenate([both, both], 0), 1, 0))
    r = 1.0 / (jnp.sum(qf * msum, 1, keepdims=True) + 1.0)
    return numer * r, r


def probs_parts(q_ref, k_ref, h, j, block):
    q = q_ref[j * block : (j + 1) * block, cols(h)]
    parts = []
    for i in range(j + 1):
        k = k_ref[i * block : (i + 1) * block, cols(h)]
        s = dot(k, q, 1, 1) * SCALE
        if i == j:
            shape = (block, block)
            keep = lax.broadcasted_iota(jnp.int32, shape, 0) <= lax.broadcasted_iota(jnp.int32, shape, 1)
            s = jnp.where(keep, s, -jnp.inf)
        parts.append(s)
    top = functools.reduce(jnp.maximum, [jnp.max(s, 0, keepdims=True) for s in parts])
    parts = [jnp.exp(s - top) for s in parts]
    r = 1.0 / sum(jnp.sum(e, 0, keepdims=True) for e in parts)
    return q, [e * r for e in parts]


def local_forward_body(heads, block, q_ref, k_ref, v_ref, o_ref):
    for h in range(heads):
        vt = v_ref[:, cols(h)].T
        for j in range(q_ref.shape[0] // block):
            _, parts = probs_parts(q_ref, k_ref, h, j, block)
            acc = sum(
                dot(vt[:, i * block : (i + 1) * block], p.astype(bf16), 1, 0) for i, p in enumerate(parts)
            )
            o_ref[j * block : (j + 1) * block, cols(h)] = acc.T


def grad_mixed_body(*refs):
    pieces, w_ref, o_ref = refs[:-2], refs[-2], refs[-1]
    x = jnp.concatenate([p[...] for p in pieces], 0)
    o_ref[...] = dot(x, w_ref[...], 1, 1).astype(bf16)


def gather_grad(count, order, grads, g_ref):
    place = lax.axis_index("tp")
    for grad, masks in zip(grads, order):
        rows = grad.shape[0] // len(masks)
        for i, m in enumerate(masks):
            spot = pl.multiple_of(flipped(place, m, count) * rows, rows)
            g_ref[pl.ds(spot, rows), :] = grad[i * rows : (i + 1) * rows, :]


def segment_memory_grad(h, qf_ref, qs_ref, qt_ref, g_ref, gate_ref, matrix, msum):
    qf = qf_ref[:, cols(h)]
    mem_out, r = read_memory(qf, qs_ref[:, pair(h)], matrix, msum)
    gmem = gate_ref[h : h + 1, :] * g_ref[:, cols(h)].astype(f32)
    gden = -jnp.sum(gmem * mem_out, 1, keepdims=True) * r
    both = halves(dot(qt_ref[pair(h), :], side(*split(gmem * r)), 1, 0))
    return (both[:HD] + both[HD:]).astype(bf16), jnp.sum(gden * qf, 0, keepdims=True), mem_out


def memory_grad_first_body(group, count, order, steps, *refs):
    grads, (qf_ref, qs_ref, qt_ref, gate_ref) = refs[: len(order)], refs[len(order) : len(order) + 4]
    recvs = refs[len(order) + 4 : len(order) + 4 + steps] + (None,)
    o_ref, g_ref, out_ref = refs[-3:]
    gather_grad(count, order, grads, g_ref)
    sums = scan_state(False, recvs, slice(0, PAD))
    rows = []
    for h in group:
        matrix = scan_state(False, recvs, rows_of(h))
        o_ref[rows_of(h), :], row, out_ref[:, cols(h - group[0])] = segment_memory_grad(
            h, qf_ref, qs_ref, qt_ref, g_ref, gate_ref, matrix, sums[h : h + 1, :]
        )
        rows.append(row)
    o_ref[:PAD, :] = jnp.concatenate(rows + [jnp.zeros((PAD - len(rows), HD), f32)], 0).astype(bf16)


def memory_grad_second_body(first, group, first_ref, qf_ref, qs_ref, qt_ref, gate_ref, g_ref, mem_ref, o_ref, out_ref):
    cut = first_ref.shape[0]
    o_ref[:cut, :] = first_ref[...]
    rows = []
    for h in group:
        o_ref[rows_of(h), :], row, out_ref[:, cols(h - group[0])] = segment_memory_grad(
            h, qf_ref, qs_ref, qt_ref, g_ref, gate_ref, *memory_of(mem_ref, h)
        )
        rows.append(row)
    head = first_ref[:PAD, :].astype(f32)
    tail = [jnp.zeros((PAD - first - len(rows), HD), f32)]
    o_ref[:PAD, :] = jnp.concatenate([head[:first]] + rows + tail, 0).astype(bf16)


def flipped(place, mask, count):
    out = 0
    bit = 1
    while bit < count:
        own = (place // bit) % 2
        out = out + bit * ((1 - own) if mask & bit else own)
        bit *= 2
    return out


def mixed_rows(heads, count, masks, qf_ref, qs_ref, mem_ref, lo_ref, gate_ref, mix_ref, known):
    place = lax.axis_index("tp")
    rows = qf_ref.shape[0] // count
    for i, m in enumerate(masks):
        spot = pl.multiple_of(flipped(place, m, count) * rows, rows)
        for h in range(heads):
            qf, qs = qf_ref[pl.ds(spot, rows), cols(h)], qs_ref[pl.ds(spot, rows), pair(h)]
            if h in known:
                mem_out = known[h][0][pl.ds(spot, rows), cols(known[h][1])]
            else:
                mem_out = read_memory(qf, qs, *memory_of(mem_ref, h))[0]
            g = gate_ref[h : h + 1, :]
            x = g * mem_out + (1.0 - g) * lo_ref[pl.ds(spot, rows), cols(h)]
            mix_ref[i * rows : (i + 1) * rows, cols(h)] = x.astype(bf16)


def output_send_body(heads, count, masks, steps, qf_ref, qs_ref, lo_ref, gate_ref, w_ref, known_ref, *refs):
    known = {h: (known_ref, h) for h in range(known_ref.shape[1] // HD)}
    recvs, (mem_ref, send_ref, mix_ref) = refs[:steps], refs[steps:]
    cut = recvs[-2].shape[0]
    for rows in (slice(0, cut), slice(cut, mem_ref.shape[0])):
        mem_ref[rows, :] = scan_state(False, recvs, rows)
    mixed_rows(heads, count, masks, qf_ref, qs_ref, mem_ref, lo_ref, gate_ref, mix_ref, known)
    send_ref[...] = dot(mix_ref[...], w_ref[...], 1, 0).astype(bf16)


def output_keep_body(
    heads, count, masks, qf_ref, qs_ref, mem_ref, lo_ref, gate_ref, w_ref, recv_ref, low_ref, high_ref, send_ref, keep_ref, mix_ref
):
    first = low_ref.shape[1] // HD
    known = {h: (low_ref, h) if h < first else (high_ref, h - first) for h in range(heads)}
    mixed_rows(heads, count, masks, qf_ref, qs_ref, mem_ref, lo_ref, gate_ref, mix_ref, known)
    total = dot(mix_ref[...], w_ref[...], 1, 0) + recv_ref[...].astype(f32)
    half = send_ref.shape[0]
    send_ref[...] = total[:half].astype(bf16)
    keep_ref[...] = total[half:]


def output_done_body(moves, keep_ref, recv_ref, *refs):
    gqs, (out_hbm, gq_hbm, out_ref, sems) = refs[: len(moves)], refs[len(moves) :]
    copies = [
        pltpu.make_async_copy(ref, gq_hbm.at[:, spots], sems.at[n]) for n, (ref, spots) in enumerate(zip(gqs, moves))
    ]
    out_ref[...] = (keep_ref[...] + recv_ref[...].astype(f32)).astype(bf16)
    copies = [pltpu.make_async_copy(out_ref, out_hbm, sems.at[len(moves)])] + copies
    for copy in copies:
        copy.start()
    for copy in copies:
        copy.wait()


def local_backward_body(group, block, q_ref, qf_ref, qs_ref, k_ref, v_ref, g_ref, mem_ref, gate_ref, *refs):
    gq_ref, gk_ref, gv_ref = refs
    blocks = q_ref.shape[0] // block
    for n, h in enumerate(group):
        g = gate_ref[h : h + 1, :]
        kt = k_ref[:, cols(h)].T
        gk = [None] * blocks
        gv = [None] * blocks

        def add(acc, i, x):
            acc[i] = x if acc[i] is None else acc[i] + x

        gq = []
        for j in range(blocks):
            q, parts = probs_parts(q_ref, k_ref, h, j, block)
            gl = ((1.0 - g) * g_ref[j * block : (j + 1) * block, cols(h)].astype(f32)).astype(bf16)
            gps = [dot(v_ref[i * block : (i + 1) * block, cols(h)], gl, 1, 1) for i in range(j + 1)]
            delta = sum(jnp.sum(p * gp, 0, keepdims=True) for p, gp in zip(parts, gps))
            acc = None
            for i, (p, gp) in enumerate(zip(parts, gps)):
                gs = (p * (gp - delta) * SCALE).astype(bf16)
                add(gk, i, dot(gs, q, 1, 0))
                add(gv, i, dot(p.astype(bf16), gl, 1, 0))
                t = dot(kt[:, i * block : (i + 1) * block], gs, 1, 0)
                acc = t if acc is None else acc + t
            gq.append(acc.T)
        for i in range(blocks):
            gk_ref[i * block : (i + 1) * block, cols(n)] = gk[i]
            gv_ref[i * block : (i + 1) * block, cols(n)] = gv[i]
        qx = q_ref[:, cols(h)].astype(f32)
        matrix, msum = memory_of(mem_ref, h)
        mem_out, r = read_memory(qf_ref[:, cols(h)], qs_ref[:, pair(h)], matrix, msum)
        gmem = g * g_ref[:, cols(h)].astype(f32)
        gden = -jnp.sum(gmem * mem_out, 1, keepdims=True) * r
        gqf = twofold(gmem * r, matrix, True) + gden * msum
        gq_ref[:, cols(n)] = (jnp.concatenate(gq, 0) + gqf * slope(qx)).astype(bf16)


def final_part(group, k_ref, v_ref, kl_ref, vl_ref, recvs, store):
    for i, h in enumerate(group):
        kx = k_ref[:, cols(h)].astype(f32)
        matrix = scan_state(True, recvs, rows_of(h))
        msum = scan_state(True, recvs, slice(0, PAD))[h : h + 1, :]
        gkf = halves(dot(v_ref[:, cols(h)], jnp.concatenate(split(matrix), 0), 1, 1)) + msum
        store(0, i, (kl_ref[:, cols(i)] + gkf * slope(kx)).astype(bf16))
        store(1, i, (vl_ref[:, cols(i)] + twofold(feat(kx), matrix)).astype(bf16))


def final_first_body(group, steps, *refs):
    outs = refs[-2:]

    def store(n, i, x):
        outs[n][:, cols(i)] = x

    final_part(group, *refs[:4], refs[4 : 4 + steps] + (None,), store)


def final_second_body(before, group, steps, *refs):
    firsts = refs[4 + steps : 6 + steps]
    outs, parts, sems = refs[-5:-3], refs[-3:-1], refs[-1]
    copies = []

    def send(ref, out, spots, sem):
        copies.append(pltpu.make_async_copy(ref, out.at[:, spots], sem))
        copies[-1].start()

    for n in range(2):
        send(firsts[n], outs[n], slice(0, before * HD), sems.at[n, len(group)])

    def store(n, i, x):
        parts[n][:, cols(i)] = x
        send(parts[n].at[:, cols(i)], outs[n], cols(group[i]), sems.at[n, i])

    final_part(group, *refs[:4], refs[4 : 4 + steps], store)
    for copy in copies:
        copy.wait()


def swap(x, axis, bit):
    count = lax.axis_size(axis)
    return lax.ppermute(x, axis, [(i, i ^ bit) for i in range(count)])


def scan(own, axis, cut):
    count = lax.axis_size(axis)
    recvs = []
    bit = 1
    while bit < count:
        have = [own] + recvs
        shapes = [own.shape]
        ends = bit * 2 == count
        if ends:
            shapes = [(cut, HD), (own.shape[0] - cut, HD)]
        sends = [own]
        if len(have) > 1 or ends:
            body = functools.partial(add_body, len(have))
            outs = [(shape, bf16) for shape in shapes]
            sends = call(body, outs, [VM] * len(have), flops=1 << 20)(*have)
        for send in sends:
            recvs.append(swap(send, axis, bit))
        bit *= 2
    return recvs


def reverse_bits(value, count):
    out = 0
    bit = 1
    while bit < count:
        out = out * 2 + (1 if value & bit else 0)
        bit *= 2
    return out


def local(query, keys, values, beta, out_weight, cotangent):
    length, width = query.shape
    heads = width // HD
    model = out_weight.shape[1]
    tp = lax.axis_size("tp")
    block = min(256, length)
    packed = (heads * HD + PAD, HD)
    hbm = pl.BlockSpec(memory_space=pltpu.HBM)
    full = (length, width)
    first = -(-heads // 2)
    groups = [list(range(first)), list(range(first, heads))]
    cut = PAD + first * HD

    def in_hbm(*xs):
        return [pltpu.with_memory_space_constraint(x, pltpu.HBM) for x in xs]

    own, keys, values = call(
        functools.partial(own_memory_body, heads),
        [(packed, bf16), (full, bf16), (full, bf16)],
        [hbm] * 2,
        scratch=[pltpu.SemaphoreType.DMA((2, heads))],
    )(*in_hbm(keys, values))
    query, feats, feats_s, feats_t, gates = call(
        functools.partial(load_query_body, heads),
        [(full, bf16), (full, f32), ((length, 2 * width), bf16), ((2 * width, length), bf16), ((-(-heads // 8) * 8, HD), f32)],
        [hbm] * 2,
        scratch=[pltpu.SMEM((heads,), f32), pltpu.SemaphoreType.DMA((heads + 1,))],
        flops=1 << 16,
    )(*in_hbm(query, beta))
    fwd = scan(own, "seq", cut)

    held = {0: cotangent}
    order, later = [[0]], []
    if tp > 1:
        held[1] = swap(cotangent, "tp", 1)
        order = [[0, 1]]
    bit = 2
    far = [0]
    while bit < tp:
        for m in list(far):
            held[m | bit] = swap(held[m], "tp", bit)
            far.append(m | bit)
        bit *= 2
    for m in far[1:]:
        held[m | 1] = swap(held[m], "tp", 1)
        later += [m, m | 1]
    order += [later] if later else []

    local_out = call(
        functools.partial(local_forward_body, heads, block), [(full, f32)], [VM, VM, VM]
    )(query, keys, values)[0]

    grads = []
    for masks in order:
        rows = cotangent.shape[0] * len(masks)
        grads.append(
            call(
                grad_mixed_body, [((rows, width), bf16)], [VM] * (len(masks) + 1)
            )(*[held[m] for m in masks], out_weight)[0]
        )

    places = [reverse_bits(tp - 1 - i, tp) for i in range(tp)]
    half = tp // 2
    steps = len(fwd)
    part, grad, low = call(
        functools.partial(memory_grad_first_body, groups[0], tp, order, steps - 1),
        [((cut, HD), bf16), (full, bf16), ((length, first * HD), f32)],
        [VM] * (len(order) + 3 + steps),
    )(*grads, feats, feats_s, feats_t, gates, *fwd[:-1])
    memory, send = call(
        functools.partial(output_send_body, heads, tp, places[:half], steps),
        [(packed, f32), ((length // 2, model), bf16)],
        [VM] * (6 + steps),
        scratch=[pltpu.VMEM((length // 2, width), bf16)],
    )(feats, feats_s, local_out, gates, out_weight, low, *fwd)
    recv = swap(send, "tp", 1)
    memory_grad, high = call(
        functools.partial(memory_grad_second_body, first, groups[1]),
        [(packed, bf16), ((length, len(groups[1]) * HD), f32)],
        [VM] * 7,
    )(part, feats, feats_s, feats_t, gates, grad, memory)
    bwd = scan(memory_grad, "seq", cut)

    quarter = length // 4
    send, keep = call(
        functools.partial(output_keep_body, heads, tp, places[half:]),
        [((quarter, model), bf16), ((quarter, model), f32)],
        [VM] * 9,
        scratch=[pltpu.VMEM((length // 2, width), bf16)],
    )(feats, feats_s, memory, local_out, gates, out_weight, recv, low, high)
    bit = 2
    while 2 * bit < tp:
        total = keep + swap(send, "tp", bit).astype(f32)
        part = total.shape[0] // 2
        send, keep = total[:part].astype(bf16), total[part:]
        bit *= 2
    recv = swap(send, "tp", bit)
    pieces = []
    for group in groups:
        part = (length, len(group) * HD)
        pieces.append(
            call(
                functools.partial(local_backward_body, group, block), [(part, bf16), (part, f32), (part, f32)], [VM] * 8
            )(query, feats, feats_s, keys, values, grad, memory, gates)
        )
    own_rows = (length // tp, model)
    output, grad_query = call(
        functools.partial(output_done_body, [slice(g[0] * HD, (g[-1] + 1) * HD) for g in groups]),
        [(own_rows, bf16), (full, bf16)],
        [VM] * (2 + len(groups)),
        out_specs=[hbm] * 2,
        scratch=[pltpu.VMEM(own_rows, bf16), pltpu.SemaphoreType.DMA((len(groups) + 1,))],
        flops=1 << 20,
    )(keep, recv, *[piece[0] for piece in pieces])
    part = (length, first * HD)
    early = call(
        functools.partial(final_first_body, groups[0], len(bwd) - 1), [(part, bf16)] * 2, [VM] * (3 + len(bwd))
    )(keys, values, *pieces[0][1:], *bwd[:-1])
    part = (length, len(groups[1]) * HD)
    grad_keys, grad_values = call(
        functools.partial(final_second_body, first, groups[1], len(bwd)),
        [(full, bf16)] * 2,
        [VM] * (6 + len(bwd)),
        out_specs=[hbm] * 2,
        scratch=[
            pltpu.VMEM(part, bf16),
            pltpu.VMEM(part, bf16),
            pltpu.SemaphoreType.DMA((2, len(groups[1]) + 1)),
        ],
    )(keys, values, *pieces[1][1:], *bwd, *early)
    return (output, grad_query, grad_keys, grad_values)


def solution(mesh):
    in_specs = (
        P("seq", "tp"),
        P("seq", "tp"),
        P("seq", "tp"),
        P("tp"),
        P("tp", None),
        P(("seq", "tp"), None),
    )
    out_specs = (P(("seq", "tp"), None), P("seq", "tp"), P("seq", "tp"), P("seq", "tp"))

    return jax.shard_map(local, mesh=mesh, in_specs=in_specs, out_specs=out_specs, check_vma=False)
```
